32 devices in a mesh: gx: 8 (over z, core), gy: 4 (over y, x).
Axes of the slice: x: 2, y: 2, z: 4, core: 2. Of those that a mesh axis runs over, the one named last changes fastest.
Arguments:
- features: float32 [8, 4, 128, 256], P('gx', 'gy'), may hold values from -6 to 6
- offsets: float32 [8, 4, 3, 128], P('gx', 'gy'), may hold values from 0 to 1
- species: int32 [8, 4, 128], P('gx', 'gy'), may hold values from 0 to 63
- neighbours: int32 [8, 4, 128, 8], P('gx', 'gy'), may hold values from 0 to 4095, as said below
- edge_mask: int32 [8, 4, 128, 8], P('gx', 'gy'), may hold values 0 or 1
- wavevectors: int32 [3, 512], replicated, may hold values from -4 to 3, as said below
- value_weight: float32 [256, 256], replicated, may hold values from -0.375 to 0.375
- radial_weight: float32 [64, 256], replicated, may hold values from -3 to 3
- species_embed: float32 [64, 256], replicated, may hold values from -3 to 3
- mixing_weight: float32 [256, 256], replicated, may hold values from -0.375 to 0.375
- group_filter: float32 [8, 256, 256], P('gx'), may hold values from -0.375 to 0.375
Outputs:
- updated: float32 [8, 4, 128, 256], P('gx', 'gy')
The draws below stay inside these ranges and needn't reach their ends.
Inputs may be any that keep to these rules, and one draw needn't show every extreme that they name: `neighbours`: every listed neighbour lies in a block whose first index differs from the atom's by at most one modulo 8 and whose second index differs by at most one modulo 4. `wavevectors`: the first component lies in -4 .. 3, the second in -2 .. 1, the third in -2 .. 2.
All inputs are finite; a program needn't handle non-finite values. No bound on the sum of `edge_mask` on one device may be relied on, other than what follows from the above.
Results may differ from the reference program's by a relative error of at most 0.0003.
Values sent between devices are 32-bit elements; how exact they have to be, the bound alone decides.
No kernel may reach another device: no remote copies, remote signals or barrier semaphores. Data moves between devices by JAX's collectives and lax.ppermute only.
A program may use at most 64 MiB of HBM per device.

```python
import math
import jax
import jax.numpy as jnp
from jax import lax

CHANNELS = 256
RADIAL = 64
SPECIES = 64
NEIGHBOUR_SLOTS = 8
MODE_COUNT = 512
ATOM_DEV = 128
LATERAL_BLOCKS = 8
TRANSVERSE_BLOCKS = 4
GROUPS = 8
GROUP_MODES = 64
ATOM_COUNT = 4096


def draw_neighbours(key, part):
    lateral_key, transverse_key, atom_key = jax.random.split(key, 3)
    shape = (LATERAL_BLOCKS, TRANSVERSE_BLOCKS, ATOM_DEV, NEIGHBOUR_SLOTS)
    lateral_shift = jax.random.randint(lateral_key, shape, -1, 2)
    transverse_shift = jax.random.randint(transverse_key, shape, -1, 2)
    chosen = jax.random.randint(atom_key, shape, 0, ATOM_DEV)
    lateral_block = jnp.arange(LATERAL_BLOCKS, dtype=jnp.int32)[:, None, None, None]
    transverse_block = jnp.arange(TRANSVERSE_BLOCKS, dtype=jnp.int32)[None, :, None, None]
    source_lateral = jnp.remainder(lateral_block + lateral_shift, LATERAL_BLOCKS)
    source_transverse = jnp.remainder(transverse_block + transverse_shift, TRANSVERSE_BLOCKS)
    return ((source_lateral * TRANSVERSE_BLOCKS + source_transverse) * ATOM_DEV + chosen).astype(jnp.int32)


def draw_wavevectors(key, part):
    lateral_key, transverse_key, vertical_key = jax.random.split(key, 3)
    lateral_half = LATERAL_BLOCKS // 2
    transverse_half = TRANSVERSE_BLOCKS // 2
    lateral_part = jax.random.randint(lateral_key, (MODE_COUNT,), -lateral_half, lateral_half)
    transverse_part = jax.random.randint(transverse_key, (MODE_COUNT,), -transverse_half, transverse_half)
    vertical_part = jax.random.randint(vertical_key, (MODE_COUNT,), -2, 3)
    return jnp.stack([lateral_part, transverse_part, vertical_part]).astype(jnp.int32)


def set_ends(entries, rng, low, top_value):
    place = [jax.random.randint(jax.random.fold_in(rng, axis), (), 0, length) for axis, length in enumerate(entries.shape)]
    widest = entries.shape.index(max(entries.shape))
    beside = place[:widest] + [(place[widest] + 1) % entries.shape[widest]] + place[widest + 1:]
    return entries.at[tuple(place)].set(low).at[tuple(beside)].set(top_value)


def steps_of(own_key, extent, cuts, low, top_value):
    def one(dim, shards_of):
        draws = jax.random.uniform(jax.random.fold_in(jax.random.fold_in(own_key, 6), dim), (shards_of,), jnp.float32, low / len(cuts), top_value / len(cuts))
        return jnp.repeat(jnp.exp(draws), extent[dim] // shards_of).reshape((-1,) + (1,) * (len(extent) - dim - 1))

    gain = one(*cuts[0])
    for cut in cuts[1:]:
        gain = gain * one(*cut)
    return gain


def gaussian(key, shape, deviation, limit, pieces=(), kind=jnp.bfloat16):
    result = jax.random.normal(key, shape, jnp.float32) * deviation
    if len(pieces) > 0:
        result = steps_of(key, shape, pieces, -0.22, 0.18) * result
    return jnp.clip(result, min=-limit, max=limit).astype(kind)


def setup_inputs(seed: int = 0) -> dict:
    keys = jax.random.split(jax.random.key(seed), 12)
    features = gaussian(keys[0], (LATERAL_BLOCKS, TRANSVERSE_BLOCKS, ATOM_DEV, CHANNELS), 1.0, 6.0, ((0, 8), (1, 4)), jnp.float32)
    offsets = jnp.clip(1.0 * jax.random.uniform(keys[1], (LATERAL_BLOCKS, TRANSVERSE_BLOCKS, 3, ATOM_DEV), jnp.float32) ** steps_of(keys[1], (LATERAL_BLOCKS, TRANSVERSE_BLOCKS, 3, ATOM_DEV), ((0, 8), (1, 4)), -0.2, 0.2), 0.0, 1.0)
    species = set_ends(jax.random.randint(keys[2], (LATERAL_BLOCKS, TRANSVERSE_BLOCKS, ATOM_DEV), 0, SPECIES), jax.random.fold_in(keys[2], 1), 0, SPECIES - 1).astype(jnp.int32)
    neighbours = draw_neighbours(jax.random.fold_in(keys[11], 71), 0)
    edge_mask = set_ends((jax.random.randint(keys[4], (LATERAL_BLOCKS, TRANSVERSE_BLOCKS, ATOM_DEV, NEIGHBOUR_SLOTS), 0, 4) < 3).astype(jnp.int32), jax.random.fold_in(keys[4], 1), 0, 1)
    wavevectors = draw_wavevectors(jax.random.fold_in(keys[11], 71), 0)
    value_weight = gaussian(keys[6], (CHANNELS, CHANNELS), CHANNELS ** -0.5, 0.375, (), jnp.float32)
    radial_weight = gaussian(keys[7], (RADIAL, CHANNELS), 4 ** -0.5, 3.0, (), jnp.float32)
    species_embed = gaussian(keys[8], (SPECIES, CHANNELS), 0.5, 3.0, (), jnp.float32)
    mixing_weight = gaussian(keys[9], (CHANNELS, CHANNELS), CHANNELS ** -0.5, 0.375, (), jnp.float32)
    group_filter = gaussian(keys[10], (GROUPS, CHANNELS, CHANNELS), CHANNELS ** -0.5, 0.375, ((0, 8),), jnp.float32)
    return {"features": features, "offsets": offsets, "species": species, "neighbours": neighbours, "edge_mask": edge_mask, "wavevectors": wavevectors, "value_weight": value_weight, "radial_weight": radial_weight, "species_embed": species_embed, "mixing_weight": mixing_weight, "group_filter": group_filter}


FULL_TURN = 2.0 * math.pi
SMEARING = 0.01
RADIAL_REACH = 3.0
SOFTEN = 0.01
HIGHEST = lax.Precision.HIGHEST

def radial(distance, basis_count):
    centres = jnp.arange(basis_count, dtype=jnp.float32) * (RADIAL_REACH / (basis_count - 1))
    spread = 2.0 * RADIAL_REACH / (basis_count - 1)
    scaled = (distance[..., None] - centres) / spread
    return jnp.exp(-scaled * scaled)

def phase_table(vectors, lateral_block, transverse_block, offsets_block, lateral_span, transverse_span):
    weights = vectors.astype(jnp.float32)
    lateral_whole = jnp.remainder(vectors[0] * lateral_block, lateral_span).astype(jnp.float32)
    transverse_whole = jnp.remainder(vectors[1] * transverse_block, transverse_span).astype(jnp.float32)
    fractions = (lateral_whole[None, :] + offsets_block[0][:, None] * weights[0][None, :]) / lateral_span
    fractions = fractions + (transverse_whole[None, :] + offsets_block[1][:, None] * weights[1][None, :]) / transverse_span
    fractions = fractions + offsets_block[2][:, None] * weights[2][None, :]
    return FULL_TURN * fractions

def damping(vectors, lateral_span, transverse_span):
    weights = vectors.astype(jnp.float32)
    lateral_wave = FULL_TURN * weights[0] / lateral_span
    transverse_wave = FULL_TURN * weights[1] / transverse_span
    vertical_wave = FULL_TURN * weights[2]
    return jnp.exp(-SMEARING * (lateral_wave * lateral_wave + transverse_wave * transverse_wave + vertical_wave * vertical_wave))

def edge_messages(nearby_values, nearby_offsets, own_position, lateral_shift, transverse_shift, keep_mask, own_embed, nearby_embed, radial_weight, mixing_weight):
    lateral_gap = lateral_shift.astype(jnp.float32) + nearby_offsets[..., 0] - own_position[:, None, 0]
    transverse_gap = transverse_shift.astype(jnp.float32) + nearby_offsets[..., 1] - own_position[:, None, 1]
    vertical_gap = nearby_offsets[..., 2] - own_position[:, None, 2]
    distance = jnp.sqrt(lateral_gap * lateral_gap + transverse_gap * transverse_gap + vertical_gap * vertical_gap + SOFTEN)
    basis = radial(distance, radial_weight.shape[0])
    basis_rows = basis.reshape(-1, basis.shape[-1])
    before = jnp.dot(basis_rows, radial_weight, precision=HIGHEST, preferred_element_type=jnp.float32).reshape(nearby_values.shape)
    hidden = jax.nn.silu(before + own_embed[:, None, :] + nearby_embed)
    filters = jnp.dot(hidden.reshape(-1, hidden.shape[-1]), mixing_weight, precision=HIGHEST, preferred_element_type=jnp.float32).reshape(nearby_values.shape)
    messages = filters * nearby_values * keep_mask.astype(jnp.float32)[..., None]
    return lax.optimization_barrier(jnp.sum(messages, axis=1)) / math.sqrt(nearby_values.shape[1])

def contract_atoms(table, feats):
    return lax.dot_general(table, feats, (((0,), (0,)), ((), ())), precision=HIGHEST, preferred_element_type=jnp.float32)

def reference(features, offsets, species, neighbours, edge_mask, wavevectors, value_weight, radial_weight, species_embed, mixing_weight, group_filter):
    lateral_span = LATERAL_BLOCKS
    transverse_span = TRANSVERSE_BLOCKS
    block_total = lateral_span * transverse_span
    channel_count = features.shape[-1]
    block_features = features.reshape(block_total, ATOM_DEV, channel_count)
    block_offsets = offsets.reshape(block_total, 3, ATOM_DEV)
    block_species = species.reshape(block_total, ATOM_DEV)
    block_neighbours = neighbours.reshape(block_total, ATOM_DEV, NEIGHBOUR_SLOTS)
    block_masks = edge_mask.reshape(block_total, ATOM_DEV, NEIGHBOUR_SLOTS)
    values = jnp.dot(features.reshape(-1, channel_count), value_weight, precision=HIGHEST, preferred_element_type=jnp.float32)
    positions = jnp.transpose(block_offsets, (0, 2, 1)).reshape(-1, 3)
    atom_embed = species_embed[species.reshape(-1)]
    block_index = jnp.arange(block_total, dtype=jnp.int32)

    def accumulate(running, inputs):
        which, feats, offsets_block = inputs
        angles = phase_table(wavevectors, which // transverse_span, which % transverse_span, offsets_block, lateral_span, transverse_span)
        partial_sum = jnp.concatenate([contract_atoms(jnp.cos(angles), feats), contract_atoms(jnp.sin(angles), feats)], axis=1)
        return (running + partial_sum, None)
    structure, unused = lax.scan(accumulate, jnp.zeros((MODE_COUNT, 2 * channel_count), jnp.float32), (block_index, block_features, block_offsets))
    grouped = structure.reshape(GROUPS, GROUP_MODES, 2, channel_count)
    mixed = jnp.einsum('gmcf,gfh->gmch', grouped, group_filter, precision=HIGHEST, preferred_element_type=jnp.float32)
    filtered = damping(wavevectors, lateral_span, transverse_span)[:, None] * mixed.reshape(MODE_COUNT, 2 * channel_count)
    scale = 1.0 / math.sqrt(ATOM_COUNT * MODE_COUNT)

    def per_block(inputs):
        which, offsets_block, kinds, listed, keep_mask = inputs
        lateral_block = which // transverse_span
        transverse_block = which % transverse_span
        angles = phase_table(wavevectors, lateral_block, transverse_block, offsets_block, lateral_span, transverse_span)
        distant = jnp.dot(jnp.cos(angles), filtered[:, :channel_count], precision=HIGHEST, preferred_element_type=jnp.float32)
        distant = distant + jnp.dot(jnp.sin(angles), filtered[:, channel_count:], precision=HIGHEST, preferred_element_type=jnp.float32)
        distant = distant * scale
        source_block = listed // ATOM_DEV
        lateral_shift = jnp.remainder(source_block // transverse_span - lateral_block + 1, lateral_span) - 1
        transverse_shift = jnp.remainder(source_block % transverse_span - transverse_block + 1, transverse_span) - 1
        own_embed = species_embed[kinds]
        nearby = edge_messages(values[listed], positions[listed], jnp.transpose(offsets_block), lateral_shift, transverse_shift, keep_mask, own_embed, atom_embed[listed], radial_weight, mixing_weight)
        return nearby + distant
    updated = lax.map(per_block, (block_index, block_offsets, block_species, block_neighbours, block_masks))
    return updated.reshape(lateral_span, transverse_span, ATOM_DEV, channel_count)
```

```python
import functools
import math

import jax
import jax.numpy as jnp
import numpy as np
from jax import lax
from jax.experimental import pallas as pl
from jax.experimental.pallas import tpu as pltpu
from jax.sharding import PartitionSpec as P


FULL_TURN = 2.0 * math.pi
SMEARING = 0.01
RADIAL_REACH = 3.0
SOFTEN = 0.01
F32 = jnp.float32
BF16 = jnp.bfloat16
EXTRA = 8
NN = (((1,), (0,)), ((), ()))
NT = (((1,), (1,)), ((), ()))


def series(function):
    nodes = 0.125 + 0.125 * np.cos(np.pi * (np.arange(64) + 0.5) / 64)
    fit = np.polynomial.chebyshev.Chebyshev.fit(nodes, function(np.sqrt(nodes)), 8, domain=[0, 0.25])
    return [float(c) for c in fit.convert(kind=np.polynomial.Polynomial).coef]


COSINE = series(lambda r: np.cos(2 * np.pi * r))
SINE = series(lambda r: np.sin(2 * np.pi * r) / r)


def horner(coefficients, z):
    total = jnp.full_like(z, coefficients[-1])
    for c in coefficients[-2::-1]:
        total = total * z + c
    return total


def cos_sin(turns):
    r = turns - jnp.floor(turns + 0.5)
    z = r * r
    return horner(COSINE, z), horner(SINE, z) * r


def dot(a, b, dims=NN):
    return lax.dot_general(a, b, dims, preferred_element_type=F32)


def split(x):
    high = x.astype(BF16)
    return high, (x - high.astype(F32)).astype(BF16)


def dot3(a, b):
    a_high, a_low = a
    b_high, b_low = b
    return dot(a_high, b_high) + dot(a_low, b_high) + dot(a_high, b_low)


def quotient(x, n):
    return jnp.floor((x + 0.5) * (1.0 / n))


def iota(shape, dim):
    return lax.broadcasted_iota(jnp.int32, shape, dim)


def component(block, atoms, channels, which):
    row, lane = divmod(which * atoms, channels)
    return block[atoms + row : atoms + row + 1, lane : lane + atoms]


def mode_columns(vectors, picks):
    rows, modes = picks.shape[0], vectors.shape[1]
    chosen = (iota((rows, modes), 1).astype(F32) == picks).astype(BF16)
    padded = jnp.concatenate([vectors, jnp.zeros((5, modes), F32)], axis=0).astype(BF16)
    triples = dot(chosen, padded, NT)
    return [triples[:, n : n + 1] for n in range(3)]


def structure_kernel(sizes, packed_ref, vectors_ref, *outs):
    atoms, channels, span0, span1, group, share = sizes
    pieces, (cos_ref, sin_ref) = outs[:span0], outs[span0:]
    lateral = lax.axis_index("gx").astype(F32)
    transverse = lax.axis_index("gy").astype(F32)
    count = span0 * share
    number = iota((count, 1), 0).astype(F32)
    turn = quotient(number, share)
    owner = lateral + turn
    owner = owner - span0 * quotient(owner, span0)
    picks = owner * group + transverse * share + (number - turn * share)
    n0, n1, n2 = mode_columns(vectors_ref[...].astype(F32), picks)
    whole0 = n0 * lateral
    whole0 = (whole0 - span0 * quotient(whole0, span0)) * (1.0 / span0)
    n0 = n0 * (1.0 / span0)
    scaled1 = n1 * (1.0 / span1)
    for block in range(span1):
        packed = packed_ref[block]
        whole1 = n1 * float(block)
        whole1 = (whole1 - span1 * quotient(whole1, span1)) * (1.0 / span1)
        u = [component(packed, atoms, channels, n) for n in range(3)]
        turns = whole0 + whole1 + n0 * u[0] + scaled1 * u[1] + n2 * u[2]
        cosine, sine = cos_sin(turns)
        cos_ref[:, block * atoms : (block + 1) * atoms] = cosine
        sin_ref[:, block * atoms : (block + 1) * atoms] = sine
    features = split(
        jnp.concatenate([packed_ref[block, :atoms] for block in range(span1)], axis=0)
    )
    cosines = dot3(split(cos_ref[...]), features)
    sines = dot3(split(sin_ref[...]), features)
    for turn in range(span0):
        pieces[turn][:share] = cosines[turn * share : (turn + 1) * share]
        pieces[turn][share:] = sines[turn * share : (turn + 1) * share]


def table_kernel(sizes, cos_ref, sin_ref, high_ref, low_ref):
    atoms, channels, span0, span1, group, share = sizes
    count = span0 * share
    for ref, lane in ((cos_ref, 0), (sin_ref, count)):
        for block in range(span1):
            rows = slice(block * atoms, (block + 1) * atoms)
            high, low = split(jnp.transpose(ref[:, rows]))
            high_ref[rows, lane : lane + count] = high
            low_ref[rows, lane : lane + count] = low


def filter_kernel(sizes, *refs):
    atoms, channels, span0, span1, group, share = sizes
    pieces, (weight_ref, vectors_ref, out_ref) = refs[:span0], refs[span0:]
    total = pieces[0][...]
    for piece in pieces[1:]:
        total = total + piece[...]
    lateral = lax.axis_index("gx").astype(F32)
    transverse = lax.axis_index("gy").astype(F32)
    rows = max(share, 8)
    picks = lateral * group + transverse * share + iota((rows, 1), 0).astype(F32)
    n0, n1, n2 = mode_columns(vectors_ref[...].astype(F32), picks)
    waves = (FULL_TURN * n0 / span0, FULL_TURN * n1 / span1, FULL_TURN * n2)
    damp = jnp.exp(-SMEARING * sum(w * w for w in waves))[:share]
    mixed = dot3(split(total), split(weight_ref[0]))
    out_ref[:share] = damp * mixed[:share]
    out_ref[share:] = damp * mixed[share:]


def project_kernel(sizes, scale, *refs):
    atoms, channels, span0, span1, group, share = sizes
    pieces, (high_ref, low_ref), outs = refs[:span0], refs[span0 : span0 + 2], refs[span0 + 2 :]
    outs, all_ref = outs[:span1], outs[span1]
    filtered = split(
        jnp.concatenate(
            [piece[:share] for piece in pieces] + [piece[share:] for piece in pieces], axis=0
        )
        * scale
    )
    everything = dot3((high_ref[...], low_ref[...]), filtered)
    all_ref[...] = everything.reshape(span1, atoms, channels)
    transverse = lax.axis_index("gy")
    for turn in range(span1):
        block = lax.rem(transverse + turn, span1)
        outs[turn][...] = all_ref[block]


def edge_kernel(
    sizes,
    relative,
    own_ref,
    before_ref,
    after_ref,
    listed_ref,
    mask_ref,
    value_ref,
    radial_ref,
    embed_ref,
    mixing_ref,
    out_ref,
    feature_scratch,
    place_scratch,
    hot_scratch,
):
    atoms, channels, span0, span1, slots, basis_count, kinds, lanes = sizes
    lateral = lax.axis_index("gx").astype(F32)
    transverse = lax.axis_index("gy")
    low_lane = iota((lanes, atoms), 0)
    own_rows = None
    for r, ref in enumerate((before_ref, own_ref, after_ref)):
        for d in range(3):
            block = d if relative else lax.rem(transverse + (d + span1 - 1), span1)
            packed = ref[block]
            at = (r * 3 + d) * atoms
            feature_scratch[at : at + atoms] = packed[:atoms]
            place = jnp.where(
                low_lane - basis_count == component(packed, atoms, channels, 3).astype(jnp.int32),
                1.0,
                0.0,
            )
            if r == 1 and d == 1:
                own_rows = place
            for n, shift in enumerate((r - 1.0, d - 1.0, 0.0)):
                u = component(packed, atoms, channels, n)
                if r == 1 and d == 1:
                    own_rows = jnp.where(low_lane == n, u, own_rows)
                rest = u + shift
                for piece in range(3):
                    part = rest.astype(BF16).astype(F32)
                    place = jnp.where(low_lane == n + 4 * piece, part, place)
                    rest = rest - part
            place_scratch[:, at : at + atoms] = place.astype(BF16)

    own = jnp.transpose(own_rows)
    lane = iota((atoms, lanes), 1)
    own_place = jnp.where(lane < 3, own, 0.0)
    first = split(jnp.concatenate([radial_ref[...], embed_ref[...]], axis=0))
    own_kind = jnp.where(lane >= basis_count, own, 0.0).astype(BF16)
    own_before = dot(own_kind, first[0]) + dot(own_kind, first[1])

    listed = listed_ref[...].astype(F32)
    source = quotient(listed, atoms)
    source0 = quotient(source, span1)
    shift0 = source0 - lateral + 1.0
    shift0 = shift0 - span0 * quotient(shift0, span0)
    shift1 = source - source0 * span1 - transverse.astype(F32) + 1.0
    shift1 = shift1 - span1 * quotient(shift1, span1)
    row = (shift0 * 3.0 + shift1) * atoms + (listed - source * atoms)
    row = jnp.where(mask_ref[...] != 0, row, -1.0).astype(jnp.int32)
    table_rows = 9 * atoms
    for slot in range(slots):
        hot = iota((atoms, table_rows), 1) == row[:, slot : slot + 1]
        hot_scratch[slot * atoms : (slot + 1) * atoms] = jnp.where(hot, 1.0, 0.0).astype(BF16)

    values = split(dot3(split(feature_scratch[...]), split(value_ref[...])))
    mixing = split(mixing_ref[...])
    centres = lane.astype(F32) * (RADIAL_REACH / (basis_count - 1))
    spread = 2.0 * RADIAL_REACH / (basis_count - 1)
    chunk = slots // 2
    total = jnp.zeros((atoms, channels), F32)
    for start in range(0, slots, chunk):
        rows = chunk * atoms
        hot = hot_scratch[start * atoms : start * atoms + rows]
        near_values = dot(hot, values[0]) + dot(hot, values[1])
        place = dot(hot, place_scratch[...], NT)
        gap = place + pltpu.roll(place, lanes - 4, 1) + pltpu.roll(place, lanes - 8, 1)
        gap = gap.reshape(chunk, atoms, lanes) - own_place[None]
        gap = jnp.where((lane < 3)[None], gap, 0.0)
        distance = jnp.sqrt(jnp.sum(gap * gap, axis=2, keepdims=True) + SOFTEN)
        scaled = (distance - centres[None]) * (1.0 / spread)
        inner = jnp.where(
            (lane < basis_count)[None],
            jnp.exp(-scaled * scaled),
            place.reshape(chunk, atoms, lanes),
        ).reshape(rows, lanes)
        before = dot3(split(inner), first).reshape(chunk, atoms, channels) + own_before[None]
        hidden = (before / (1.0 + jnp.exp(-before))).reshape(rows, channels)
        filters = dot3(split(hidden), mixing)
        total = total + jnp.sum((filters * near_values).reshape(chunk, atoms, channels), axis=0)
    out_ref[...] = total * (1.0 / math.sqrt(slots))


def call(kernel, out_shape, operands, flops, scratch=()):
    moved = sum(x.size * 4 for x in operands)
    return pl.pallas_call(
        kernel,
        out_shape=out_shape,
        scratch_shapes=list(scratch),
        cost_estimate=pl.CostEstimate(flops=flops, bytes_accessed=moved, transcendentals=0),
    )(*operands)


def shift(x, axis, by):
    count = lax.axis_size(axis)
    return lax.ppermute(x, axis, [(i, (i + by) % count) for i in range(count)])


def shards(
    features,
    offsets,
    species,
    neighbours,
    edge_mask,
    wavevectors,
    value_weight,
    radial_weight,
    species_embed,
    mixing_weight,
    group_filter,
):
    span0 = lax.axis_size("gx")
    span1 = lax.axis_size("gy")
    atoms, channels = features.shape[2:]
    slots = neighbours.shape[3]
    modes = wavevectors.shape[1]
    basis_count, kinds = radial_weight.shape[0], species_embed.shape[0]
    group = modes // span0
    share = group // span1
    sizes = (atoms, channels, span0, span1, group, share)
    count = span0 * share

    carried = jnp.concatenate([offsets[0, 0], species[0, 0].astype(F32)[None]], axis=0)
    carried = carried.reshape(-1, channels)
    packed = jnp.concatenate(
        [features[0, 0], carried, jnp.zeros((EXTRA - carried.shape[0], channels), F32)], axis=0
    )
    column = lax.all_gather(packed, "gy", axis=0, tiled=False)
    relative = span1 > 4
    near = column
    if relative:
        here = lax.axis_index("gy")
        near = jnp.stack(
            [
                lax.dynamic_index_in_dim(column, (here + d) % span1, 0, keepdims=False)
                for d in (-1, 0, 1)
            ]
        )

    piece = jax.ShapeDtypeStruct((2 * share, channels), F32)
    wide = jax.ShapeDtypeStruct((count, span1 * atoms), F32)
    *pieces, cosines, sines = call(
        functools.partial(structure_kernel, sizes),
        [piece] * span0 + [wide] * 2,
        (column, wavevectors),
        12 * count * span1 * atoms * channels,
    )
    received = [pieces[0]] + [shift(pieces[k], "gx", k) for k in range(1, span0)]
    from_before = shift(near, "gx", 1)
    from_after = shift(near, "gx", -1)

    table = jax.ShapeDtypeStruct((span1 * atoms, 2 * count), BF16)
    high, low = call(
        functools.partial(table_kernel, sizes), [table] * 2, (cosines, sines), 10**8
    )

    filtered = call(
        functools.partial(filter_kernel, sizes),
        piece,
        (*received, group_filter, wavevectors),
        12 * share * channels * channels,
    )
    gathered = [filtered] + [shift(filtered, "gx", -k) for k in range(1, span0)]

    lanes = -(-(basis_count + kinds) // 128) * 128
    edge_sizes = (atoms, channels, span0, span1, slots, basis_count, kinds, lanes)
    nearby = call(
        functools.partial(edge_kernel, edge_sizes, relative),
        jax.ShapeDtypeStruct((atoms, channels), F32),
        (
            near,
            from_before,
            from_after,
            neighbours[0, 0],
            edge_mask[0, 0],
            value_weight,
            radial_weight,
            species_embed,
            mixing_weight,
        ),
        4 * 10**9,
        (
            pltpu.VMEM((9 * atoms, channels), F32),
            pltpu.VMEM((lanes, 9 * atoms), BF16),
            pltpu.VMEM((slots * atoms, 9 * atoms), BF16),
        ),
    )

    block = jax.ShapeDtypeStruct((atoms, channels), F32)
    scale = 1.0 / math.sqrt(atoms * span0 * span1 * modes)
    distant = call(
        functools.partial(project_kernel, sizes, scale),
        [block] * span1,
        (*gathered, high, low),
        12 * count * span1 * atoms * channels,
        (pltpu.VMEM((span1, atoms, channels), F32),),
    )
    total = nearby + distant[0]
    for k in range(1, span1):
        total = total + shift(distant[k], "gy", k)
    return total[None, None]


def solution(mesh):
    placed = (
        P("gx", "gy", None, None),
        P("gx", "gy", None, None),
        P("gx", "gy", None),
        P("gx", "gy", None, None),
        P("gx", "gy", None, None),
        P(),
        P(),
        P(),
        P(),
        P(),
        P("gx", None, None),
    )
    return jax.shard_map(
        shards, mesh=mesh, in_specs=placed, out_specs=P("gx", "gy", None, None), check_vma=False
    )
```

```python
import functools
import math

import jax
import jax.numpy as jnp
import numpy as np
from jax import lax
from jax.experimental import pallas as pl
from jax.experimental.pallas import tpu as pltpu
from jax.sharding import PartitionSpec as P


FULL_TURN = 2.0 * math.pi
SMEARING = 0.01
RADIAL_REACH = 3.0
SOFTEN = 0.01
F32 = jnp.float32
BF16 = jnp.bfloat16
EXTRA = 8
NN = (((1,), (0,)), ((), ()))
NT = (((1,), (1,)), ((), ()))


def series(function):
    nodes = 0.125 + 0.125 * np.cos(np.pi * (np.arange(64) + 0.5) / 64)
    fit = np.polynomial.chebyshev.Chebyshev.fit(nodes, function(np.sqrt(nodes)), 8, domain=[0, 0.25])
    return [float(c) for c in fit.convert(kind=np.polynomial.Polynomial).coef]


COSINE = series(lambda r: np.cos(2 * np.pi * r))
SINE = series(lambda r: np.sin(2 * np.pi * r) / r)


def horner(coefficients, z):
    total = jnp.full_like(z, coefficients[-1])
    for c in coefficients[-2::-1]:
        total = total * z + c
    return total


def cos_sin(turns):
    r = turns - jnp.floor(turns + 0.5)
    z = r * r
    return horner(COSINE, z), horner(SINE, z) * r


def dot(a, b, dims=NN):
    return lax.dot_general(a, b, dims, preferred_element_type=F32)


def split(x):
    high = x.astype(BF16)
    return high, (x - high.astype(F32)).astype(BF16)


def dot3(a, b):
    a_high, a_low = a
    b_high, b_low = b
    return dot(a_high, b_high) + dot(a_low, b_high) + dot(a_high, b_low)


def quotient(x, n):
    return jnp.floor((x + 0.5) * (1.0 / n))


def iota(shape, dim):
    return lax.broadcasted_iota(jnp.int32, shape, dim)


def component(block, atoms, channels, which):
    row, lane = divmod(which * atoms, channels)
    return block[atoms + row : atoms + row + 1, lane : lane + atoms]


def mode_columns(vectors, picks):
    rows, modes = picks.shape[0], vectors.shape[1]
    chosen = (iota((rows, modes), 1).astype(F32) == picks).astype(BF16)
    padded = jnp.concatenate([vectors, jnp.zeros((5, modes), F32)], axis=0).astype(BF16)
    triples = dot(chosen, padded, NT)
    return [triples[:, n : n + 1] for n in range(3)]


def pack_kernel(sizes, features_ref, offsets_ref, species_ref, out_ref):
    atoms, channels = sizes[:2]
    out_ref[:atoms] = features_ref[0, 0]
    out_ref[atoms:] = jnp.zeros((EXTRA, channels), F32)
    for which in range(4):
        row, lane = divmod(which * atoms, channels)
        source = offsets_ref[0, which] if which < 3 else species_ref[0].astype(F32)
        out_ref[atoms + row : atoms + row + 1, lane : lane + atoms] = source


def structure_kernel(sizes, *refs):
    atoms, channels, span0, span1, group, share = sizes
    blocks, vectors_ref, outs = refs[:span1], refs[span1], refs[span1 + 1 :]
    pieces, (cos_ref, sin_ref) = outs[:span0], outs[span0:]
    lateral = lax.axis_index("gx").astype(F32)
    transverse = lax.axis_index("gy").astype(F32)
    count = span0 * share
    number = iota((count, 1), 0).astype(F32)
    turn = quotient(number, share)
    owner = lateral + turn
    owner = owner - span0 * quotient(owner, span0)
    picks = owner * group + transverse * share + (number - turn * share)
    n0, n1, n2 = mode_columns(vectors_ref[...].astype(F32), picks)
    whole0 = n0 * lateral
    whole0 = (whole0 - span0 * quotient(whole0, span0)) * (1.0 / span0)
    n0 = n0 * (1.0 / span0)
    scaled1 = n1 * (1.0 / span1)
    for back in range(span1):
        packed = blocks[back]
        whole1 = n1 * (transverse - back)
        whole1 = (whole1 - span1 * quotient(whole1, span1)) * (1.0 / span1)
        u = [component(packed, atoms, channels, n) for n in range(3)]
        turns = whole0 + whole1 + n0 * u[0] + scaled1 * u[1] + n2 * u[2]
        cosine, sine = cos_sin(turns)
        cos_ref[:, back * atoms : (back + 1) * atoms] = cosine
        sin_ref[:, back * atoms : (back + 1) * atoms] = sine
    features = split(jnp.concatenate([block[:atoms] for block in blocks], axis=0))
    cosines = dot3(split(cos_ref[...]), features)
    sines = dot3(split(sin_ref[...]), features)
    for turn in range(span0):
        pieces[turn][:share] = cosines[turn * share : (turn + 1) * share]
        pieces[turn][share:] = sines[turn * share : (turn + 1) * share]


def pair_kernel(before_ref, after_ref, out_ref):
    out_ref[0] = before_ref[...]
    out_ref[1] = after_ref[...]


def table_kernel(sizes, cos_ref, sin_ref, high_ref, low_ref):
    atoms, _, span0, span1, _, share = sizes
    count = span0 * share
    for ref, lane in ((cos_ref, 0), (sin_ref, count)):
        for block in range(span1):
            rows = slice(block * atoms, (block + 1) * atoms)
            high, low = split(jnp.transpose(ref[:, rows]))
            high_ref[rows, lane : lane + count] = high
            low_ref[rows, lane : lane + count] = low


def filter_kernel(sizes, *refs):
    _, _, span0, span1, group, share = sizes
    pieces, (weight_ref, vectors_ref, out_ref) = refs[:span0], refs[span0:]
    total = pieces[0][...]
    for piece in pieces[1:]:
        total = total + piece[...]
    lateral = lax.axis_index("gx").astype(F32)
    transverse = lax.axis_index("gy").astype(F32)
    rows = max(share, 8)
    picks = lateral * group + transverse * share + iota((rows, 1), 0).astype(F32)
    n0, n1, n2 = mode_columns(vectors_ref[...].astype(F32), picks)
    waves = (FULL_TURN * n0 / span0, FULL_TURN * n1 / span1, FULL_TURN * n2)
    damp = jnp.exp(-SMEARING * sum(w * w for w in waves))[:share]
    mixed = dot3(split(total), split(weight_ref[0]))
    out_ref[:share] = damp * mixed[:share]
    out_ref[share:] = damp * mixed[share:]


def project_kernel(sizes, scale, *refs):
    atoms, _, span0, span1, _, share = sizes
    pieces, (high_ref, low_ref), outs = refs[:span0], refs[span0 : span0 + 2], refs[span0 + 2 :]
    filtered = split(
        jnp.concatenate(
            [piece[:share] for piece in pieces] + [piece[share:] for piece in pieces], axis=0
        )
        * scale
    )
    everything = dot3((high_ref[...], low_ref[...]), filtered)
    for back in range(span1):
        outs[back][...] = everything[back * atoms : (back + 1) * atoms]


def edge_kernel(
    sizes,
    own_refs,
    before_ref,
    after_ref,
    left_ref,
    right_ref,
    listed_ref,
    mask_ref,
    value_ref,
    radial_ref,
    embed_ref,
    mixing_ref,
    out_ref,
    feature_scratch,
    place_scratch,
    hot_scratch,
):
    atoms, channels, span0, span1, slots, basis_count, _, lanes = sizes
    lateral = lax.axis_index("gx").astype(F32)
    transverse = lax.axis_index("gy").astype(F32)
    low_lane = iota((lanes, atoms), 0)
    own_rows = None
    table = (
        (left_ref.at[0], before_ref, right_ref.at[0]),
        own_refs,
        (left_ref.at[1], after_ref, right_ref.at[1]),
    )
    for r, row_refs in enumerate(table):
        for d, packed in enumerate(row_refs):
            at = (r * 3 + d) * atoms
            feature_scratch[at : at + atoms] = packed[:atoms]
            place = jnp.where(
                low_lane - basis_count == component(packed, atoms, channels, 3).astype(jnp.int32),
                1.0,
                0.0,
            )
            if r == 1 and d == 1:
                own_rows = place
            for n, shift in enumerate((r - 1.0, d - 1.0, 0.0)):
                u = component(packed, atoms, channels, n)
                if r == 1 and d == 1:
                    own_rows = jnp.where(low_lane == n, u, own_rows)
                rest = u + shift
                for piece in range(3):
                    part = rest.astype(BF16).astype(F32)
                    place = jnp.where(low_lane == n + 4 * piece, part, place)
                    rest = rest - part
            place_scratch[:, at : at + atoms] = place.astype(BF16)

    own = jnp.transpose(own_rows)
    lane = iota((atoms, lanes), 1)
    own_place = jnp.where(lane < 3, own, 0.0)
    first = split(jnp.concatenate([radial_ref[...], embed_ref[...]], axis=0))
    own_kind = jnp.where(lane >= basis_count, own, 0.0).astype(BF16)
    own_before = dot(own_kind, first[0]) + dot(own_kind, first[1])

    listed = listed_ref[...].astype(F32)
    source = quotient(listed, atoms)
    source0 = quotient(source, span1)
    shift0 = source0 - lateral + 1.0
    shift0 = shift0 - span0 * quotient(shift0, span0)
    shift1 = source - source0 * span1 - transverse + 1.0
    shift1 = shift1 - span1 * quotient(shift1, span1)
    row = (shift0 * 3.0 + shift1) * atoms + (listed - source * atoms)
    row = jnp.transpose(jnp.where(mask_ref[...] != 0, row, -1.0)).astype(jnp.int32)
    table_rows = 9 * atoms
    for slot in range(slots):
        hot = iota((atoms, table_rows), 1) == row[:, slot : slot + 1]
        hot_scratch[slot * atoms : (slot + 1) * atoms] = jnp.where(hot, 1.0, 0.0).astype(BF16)

    values = split(dot3(split(feature_scratch[...]), split(value_ref[...])))
    mixing = split(mixing_ref[...])
    centres = lane.astype(F32) * (RADIAL_REACH / (basis_count - 1))
    spread = 2.0 * RADIAL_REACH / (basis_count - 1)
    chunk = slots // 2
    total = jnp.zeros((atoms, channels), F32)
    for start in range(0, slots, chunk):
        rows = chunk * atoms
        hot = hot_scratch[start * atoms : start * atoms + rows]
        near_values = dot(hot, values[0]) + dot(hot, values[1])
        place = dot(hot, place_scratch[...], NT)
        gap = place + pltpu.roll(place, lanes - 4, 1) + pltpu.roll(place, lanes - 8, 1)
        gap = gap.reshape(chunk, atoms, lanes) - own_place[None]
        gap = jnp.where((lane < 3)[None], gap, 0.0)
        distance = jnp.sqrt(jnp.sum(gap * gap, axis=2, keepdims=True) + SOFTEN)
        scaled = (distance - centres[None]) * (1.0 / spread)
        inner = jnp.where(
            (lane < basis_count)[None],
            jnp.exp(-scaled * scaled),
            place.reshape(chunk, atoms, lanes),
        ).reshape(rows, lanes)
        before = dot3(split(inner), first).reshape(chunk, atoms, channels) + own_before[None]
        hidden = (before / (1.0 + jnp.exp(-before))).reshape(rows, channels)
        filters = dot3(split(hidden), mixing)
        total = total + jnp.sum((filters * near_values).reshape(chunk, atoms, channels), axis=0)
    out_ref[...] = total * (1.0 / math.sqrt(slots))


def call(kernel, out_shape, operands, flops, scratch=(), room=8):
    moved = sum(x.size * 4 for x in operands)
    return pl.pallas_call(
        kernel,
        out_shape=out_shape,
        scratch_shapes=list(scratch),
        compiler_params=pltpu.CompilerParams(vmem_limit_bytes=room * 2**20),
        cost_estimate=pl.CostEstimate(flops=flops, bytes_accessed=moved, transcendentals=0),
    )(*operands)


def shift(x, axis, by):
    count = lax.axis_size(axis)
    return lax.ppermute(x, axis, [(i, (i + by) % count) for i in range(count)])


def shards(
    features,
    offsets,
    species,
    neighbours,
    edge_mask,
    wavevectors,
    value_weight,
    radial_weight,
    species_embed,
    mixing_weight,
    group_filter,
):
    span0 = lax.axis_size("gx")
    span1 = lax.axis_size("gy")
    atoms, channels = features.shape[2:]
    slots = neighbours.shape[3]
    modes = wavevectors.shape[1]
    basis_count, kinds = radial_weight.shape[0], species_embed.shape[0]
    group = modes // span0
    share = group // span1
    sizes = (atoms, channels, span0, span1, group, share)
    count = span0 * share

    packed = call(
        functools.partial(pack_kernel, sizes),
        jax.ShapeDtypeStruct((atoms + EXTRA, channels), F32),
        (features, jnp.transpose(offsets, (0, 2, 1, 3)), species),
        10**6,
    )
    column = [packed] + [shift(packed, "gy", k) for k in range(1, span1)]
    from_before = shift(packed, "gx", 1)
    from_after = shift(packed, "gx", -1)

    piece = jax.ShapeDtypeStruct((2 * share, channels), F32)
    wide = jax.ShapeDtypeStruct((count, span1 * atoms), F32)
    *pieces, cosines, sines = call(
        functools.partial(structure_kernel, sizes),
        [piece] * span0 + [wide] * 2,
        (*column, wavevectors),
        12 * count * span1 * atoms * channels,
    )
    received = [pieces[0]] + [shift(pieces[k], "gx", k) for k in range(1, span0)]
    pair = call(
        pair_kernel, jax.ShapeDtypeStruct((2, *packed.shape), F32), (from_before, from_after), 10**6
    )
    from_left = shift(pair, "gy", 1)
    from_right = shift(pair, "gy", -1)

    table = jax.ShapeDtypeStruct((span1 * atoms, 2 * count), BF16)
    high, low = call(functools.partial(table_kernel, sizes), [table] * 2, (cosines, sines), 10**8)

    filtered = call(
        functools.partial(filter_kernel, sizes),
        piece,
        (*received, group_filter, wavevectors),
        12 * share * channels * channels,
    )
    gathered = [filtered] + [shift(filtered, "gx", -k) for k in range(1, span0)]

    lanes = -(-(basis_count + kinds) // 128) * 128
    edge_sizes = (atoms, channels, span0, span1, slots, basis_count, kinds, lanes)
    nearby = call(
        lambda left, here, right, *refs: edge_kernel(edge_sizes, (left, here, right), *refs),
        jax.ShapeDtypeStruct((atoms, channels), F32),
        (
            column[1],
            column[0],
            column[-1],
            from_before,
            from_after,
            from_left,
            from_right,
            jnp.transpose(neighbours[0, 0]),
            jnp.transpose(edge_mask[0, 0]),
            value_weight,
            radial_weight,
            species_embed,
            mixing_weight,
        ),
        4 * 10**9,
        (
            pltpu.VMEM((9 * atoms, channels), F32),
            pltpu.VMEM((lanes, 9 * atoms), BF16),
            pltpu.VMEM((slots * atoms, 9 * atoms), BF16),
        ),
        24,
    )

    block = jax.ShapeDtypeStruct((atoms, channels), F32)
    scale = 1.0 / math.sqrt(atoms * span0 * span1 * modes)
    distant = call(
        functools.partial(project_kernel, sizes, scale),
        [block] * span1,
        (*gathered, high, low),
        12 * count * span1 * atoms * channels,
    )
    total = nearby + distant[0]
    for k in range(1, span1):
        total = total + shift(distant[k], "gy", -k)
    return total[None, None]


def solution(mesh):
    placed = (
        P("gx", "gy", None, None),
        P("gx", "gy", None, None),
        P("gx", "gy", None),
        P("gx", "gy", None, None),
        P("gx", "gy", None, None),
        P(),
        P(),
        P(),
        P(),
        P(),
        P("gx", None, None),
    )
    return jax.shard_map(
        shards, mesh=mesh, in_specs=placed, out_specs=P("gx", "gy", None, None), check_vma=False
    )
```

```python
import functools
import math

import jax
import jax.numpy as jnp
import numpy as np
from jax import lax
from jax.experimental import pallas as pl
from jax.experimental.pallas import tpu as pltpu
from jax.sharding import PartitionSpec as P


FULL_TURN = 2.0 * math.pi
SMEARING = 0.01
RADIAL_REACH = 3.0
SOFTEN = 0.01
VERTICAL = 2
F32 = jnp.float32
BF16 = jnp.bfloat16
EXTRA = 8
NN = (((1,), (0,)), ((), ()))
NT = (((1,), (1,)), ((), ()))


def series(function):
    nodes = 0.125 + 0.125 * np.cos(np.pi * (np.arange(64) + 0.5) / 64)
    fit = np.polynomial.chebyshev.Chebyshev.fit(nodes, function(np.sqrt(nodes)), 8, domain=[0, 0.25])
    return [float(c) for c in fit.convert(kind=np.polynomial.Polynomial).coef]


COSINE = series(lambda r: np.cos(2 * np.pi * r))
SINE = series(lambda r: np.sin(2 * np.pi * r) / r)


def horner(coefficients, z):
    total = jnp.full_like(z, coefficients[-1])
    for c in coefficients[-2::-1]:
        total = total * z + c
    return total


def cos_sin(turns):
    r = turns - jnp.floor(turns + 0.5)
    z = r * r
    return horner(COSINE, z), horner(SINE, z) * r


def dot(a, b, dims=NN):
    return lax.dot_general(a, b, dims, preferred_element_type=F32)


def split(x):
    high = x.astype(BF16)
    return high, (x - high.astype(F32)).astype(BF16)


def dot3(a, b):
    a_high, a_low = a
    b_high, b_low = b
    return dot(a_high, b_high) + dot(a_low, b_high) + dot(a_high, b_low)


def quotient(x, n):
    return jnp.floor((x + 0.5) * (1.0 / n))


def iota(shape, dim):
    return lax.broadcasted_iota(jnp.int32, shape, dim)


def component(block, atoms, channels, which):
    row, lane = divmod(which * atoms, channels)
    return block[atoms + row : atoms + row + 1, lane : lane + atoms]


def mode_columns(vectors, picks):
    rows, modes = picks.shape[0], vectors.shape[1]
    chosen = (iota((rows, modes), 1).astype(F32) == picks).astype(BF16)
    padded = jnp.concatenate([vectors, jnp.zeros((5, modes), F32)], axis=0).astype(BF16)
    triples = dot(chosen, padded, NT)
    return [triples[:, n : n + 1] for n in range(3)]


def distinct_triples(span0, span1):
    kept = {}
    for n0 in range(-(span0 // 2), span0 - span0 // 2):
        for n1 in range(-(span1 // 2), span1 - span1 // 2):
            for n2 in range(-VERTICAL, VERTICAL + 1):
                if (-n0, -n1, -n2) not in kept:
                    kept[(n0, n1, n2)] = None
    return list(kept)


def key_of(n0, n1, n2):
    return jnp.abs(n0 + 128.0 * n1 + 16384.0 * n2)


def rows_of(basis_ref, vectors_ref, rows, parity):
    if basis_ref is None:
        picks = parity.astype(F32) * rows + iota((rows, 1), 0).astype(F32)
        return mode_columns(vectors_ref[...].astype(F32), picks)
    triples = basis_ref[parity]
    return [triples[:, n : n + 1] for n in range(3)]


def phases(sizes, triples, lateral, transverse, packed):
    atoms, channels, span0, span1 = sizes[:4]
    n0, n1, n2 = triples
    whole0 = n0 * lateral
    whole0 = (whole0 - span0 * quotient(whole0, span0)) * (1.0 / span0)
    whole1 = n1 * transverse
    whole1 = (whole1 - span1 * quotient(whole1, span1)) * (1.0 / span1)
    u = [component(packed, atoms, channels, n) for n in range(3)]
    turns = whole0 + whole1 + n0 * (1.0 / span0) * u[0] + n1 * (1.0 / span1) * u[1] + n2 * u[2]
    return cos_sin(turns)


def place():
    lateral, transverse = lax.axis_index("gx"), lax.axis_index("gy")
    parity = lax.rem(lateral, 2)
    return lateral.astype(F32), transverse.astype(F32), parity


def pack_kernel(
    sizes, features_ref, offsets_ref, species_ref, weight_ref, out_ref, rows_ref, *scratch
):
    atoms, channels, _, span1 = sizes[:4]
    offsets_scratch, species_scratch, sems = scratch
    width = channels // span1
    start = pl.multiple_of(lax.axis_index("gy") * width, math.gcd(width, 8))
    copies = [
        pltpu.make_async_copy(offsets_ref.at[0], offsets_scratch, sems.at[0]),
        pltpu.make_async_copy(species_ref.at[0], species_scratch, sems.at[1]),
        pltpu.make_async_copy(features_ref.at[0, 0], out_ref.at[0:atoms], sems.at[2]),
        pltpu.make_async_copy(weight_ref.at[0, pl.ds(start, width)], rows_ref, sems.at[3]),
    ]
    for copy in copies:
        copy.start()
    out_ref[atoms:] = jnp.zeros((EXTRA, channels), F32)
    for copy in copies[:2]:
        copy.wait()
    for which in range(4):
        row, lane = divmod(which * atoms, channels)
        source = offsets_scratch[which] if which < 3 else species_scratch[...].astype(F32)
        out_ref[atoms + row : atoms + row + 1, lane : lane + atoms] = source
    for copy in copies[2:]:
        copy.wait()


def join_kernel(*refs):
    for n, ref in enumerate(refs[:-1]):
        refs[-1][n] = ref[...]


def structure_kernel(sizes, rows, canonical, *refs):
    atoms, channels, _, span1 = sizes[:4]
    own_ref, pair_ref, vectors_ref = refs[:3]
    basis_ref, out_ref = refs[3] if canonical else None, refs[-1]
    lateral, transverse, parity = place()
    triples = rows_of(basis_ref, vectors_ref, rows, parity)
    cosines, sines, features = [], [], []
    for ref, row in ((own_ref, lateral), (pair_ref, lateral + 1.0 - 2.0 * parity.astype(F32))):
        for back in range(span1):
            packed = ref.at[back]
            cosine, sine = phases(sizes, triples, row, transverse - back, packed)
            cosines.append(cosine)
            sines.append(sine)
            features.append(packed[:atoms])
    table = jnp.concatenate(
        [jnp.concatenate(cosines, axis=1), jnp.concatenate(sines, axis=1)], axis=0
    )
    sums = dot3(split(table), split(jnp.concatenate(features, axis=0)))
    width = channels // span1
    for half in range(2):
        part = sums[half * rows : (half + 1) * rows]
        mine = jnp.zeros((rows, width), F32)
        for c in range(span1):
            mine = jnp.where(transverse == c, part[:, c * width : (c + 1) * width], mine)
        out_ref[:, half * width : (half + 1) * width] = mine


def table_kernel(sizes, rows, canonical, *refs):
    atoms, _, _, span1 = sizes[:4]
    own_ref, vectors_ref = refs[:2]
    basis_ref, (high_ref, low_ref) = refs[2] if canonical else None, refs[-2:]
    lateral, transverse, parity = place()
    sides = [rows_of(basis_ref, vectors_ref, rows, p) for p in (parity, 1 - parity)]
    for back in range(span1):
        packed = own_ref.at[back]
        parts = []
        for triples in sides:
            parts.extend(phases(sizes, triples, lateral, transverse - back, packed))
        at = slice(back * atoms, (back + 1) * atoms)
        high_ref[at], low_ref[at] = split(jnp.transpose(jnp.concatenate(parts, axis=0)))


def filter_kernel(sizes, rows, canonical, *refs):
    _, channels, span0, span1, group = sizes
    pairs = span0 // 2
    sums, (own_ref, pair_ref, vectors_ref) = refs[:pairs], refs[pairs : pairs + 3]
    basis_ref, out_ref = refs[pairs + 3] if canonical else None, refs[-1]
    lateral, _, parity = place()
    triples = rows_of(basis_ref, vectors_ref, rows, parity)
    n0, n1, n2 = triples
    waves = (FULL_TURN * n0 / span0, FULL_TURN * n1 / span1, FULL_TURN * n2)
    damp = jnp.exp(-SMEARING * sum(w * w for w in waves))

    number = iota((1, span0), 1).astype(F32)
    side = quotient(number, pairs)
    turn = number - pairs * side
    kind = parity.astype(F32)
    row = quotient(lateral, 2) + turn
    row = 2.0 * (row - pairs * quotient(row, pairs)) + jnp.where(side == 0.0, kind, 1.0 - kind)
    modes = vectors_ref.shape[1]
    if canonical:
        listed = vectors_ref[...].astype(F32)
        keys = key_of(listed[0:1], listed[1:2], listed[2:3])
        matches = (key_of(n0, n1, n2) == keys).astype(BF16)
        groups = quotient(iota((modes, span0), 0).astype(F32), group)
        counts = dot(matches, (groups == row).astype(BF16))
    else:
        picks = kind * rows + iota((rows, 1), 0).astype(F32)
        counts = (quotient(picks, group) == row).astype(F32)
    weights = counts * damp

    total = sums[0][...]
    for ref in sums[1:]:
        total = total + ref[...]
    width = channels // span1
    mixed = jnp.zeros((2 * rows, channels), F32)
    for n in range(span0):
        scaled = total * weights[:, n : n + 1]
        both = jnp.concatenate([scaled[:, :width], scaled[:, width:]], axis=0)
        weight = own_ref[n] if n < pairs else pair_ref[n - pairs]
        mixed = mixed + dot3(split(both), split(weight))
    out_ref[...] = mixed


def project_kernel(sizes, scale, own_ref, pair_ref, high_ref, low_ref, *outs):
    atoms, span1 = sizes[0], sizes[3]
    filtered = split(jnp.concatenate([own_ref[...], pair_ref[...]], axis=0) * scale)
    everything = dot3((high_ref[...], low_ref[...]), filtered)
    for back in range(span1):
        outs[back][...] = everything[back * atoms : (back + 1) * atoms]


def edge_kernel(
    sizes,
    own_ref,
    pair_ref,
    across_ref,
    left_ref,
    right_ref,
    listed_ref,
    mask_ref,
    value_ref,
    radial_ref,
    embed_ref,
    mixing_ref,
    out_ref,
    feature_scratch,
    place_scratch,
    hot_scratch,
):
    atoms, channels, span0, span1, slots, basis_count, _, lanes = sizes
    lateral, transverse, parity = place()
    toward = 1.0 - 2.0 * parity.astype(F32)
    last = span1 - 1
    low_lane = iota((lanes, atoms), 0)
    own_rows = None
    table = (
        (left_ref, across_ref, right_ref),
        (own_ref.at[1], own_ref.at[0], own_ref.at[last]),
        (pair_ref.at[1], pair_ref.at[0], pair_ref.at[last]),
    )
    for r, row_refs in enumerate(table):
        for d, packed in enumerate(row_refs):
            at = (r * 3 + d) * atoms
            feature_scratch[at : at + atoms] = packed[:atoms]
            where = jnp.where(
                low_lane - basis_count == component(packed, atoms, channels, 3).astype(jnp.int32),
                1.0,
                0.0,
            )
            if r == 1 and d == 1:
                own_rows = where
            for n, shift in enumerate(((r - 1.0) * toward, d - 1.0, 0.0)):
                u = component(packed, atoms, channels, n)
                if r == 1 and d == 1:
                    own_rows = jnp.where(low_lane == n, u, own_rows)
                rest = u + shift
                for piece in range(3):
                    part = rest.astype(BF16).astype(F32)
                    where = jnp.where(low_lane == n + 4 * piece, part, where)
                    rest = rest - part
            place_scratch[:, at : at + atoms] = where.astype(BF16)

    own = jnp.transpose(own_rows)
    lane = iota((atoms, lanes), 1)
    own_place = jnp.where(lane < 3, own, 0.0)
    first = split(jnp.concatenate([radial_ref[...], embed_ref[...]], axis=0))
    own_kind = jnp.where(lane >= basis_count, own, 0.0).astype(BF16)
    own_before = dot(own_kind, first[0]) + dot(own_kind, first[1])

    listed = listed_ref[...].astype(F32)
    source = quotient(listed, atoms)
    source0 = quotient(source, span1)
    shift0 = source0 - lateral + 1.0
    shift0 = shift0 - span0 * quotient(shift0, span0)
    shift1 = source - source0 * span1 - transverse + 1.0
    shift1 = shift1 - span1 * quotient(shift1, span1)
    line = (shift0 - 1.0) * toward + 1.0
    row = (line * 3.0 + shift1) * atoms + (listed - source * atoms)
    row = jnp.transpose(jnp.where(mask_ref[...] != 0, row, -1.0)).astype(jnp.int32)
    table_rows = 9 * atoms
    for slot in range(slots):
        hot = iota((atoms, table_rows), 1) == row[:, slot : slot + 1]
        hot_scratch[slot * atoms : (slot + 1) * atoms] = jnp.where(hot, 1.0, 0.0).astype(BF16)

    values = split(dot3(split(feature_scratch[...]), split(value_ref[...])))
    mixing = split(mixing_ref[...])
    centres = lane.astype(F32) * (RADIAL_REACH / (basis_count - 1))
    spread = 2.0 * RADIAL_REACH / (basis_count - 1)
    chunk = slots // 2
    total = jnp.zeros((atoms, channels), F32)
    for start in range(0, slots, chunk):
        rows = chunk * atoms
        hot = hot_scratch[start * atoms : start * atoms + rows]
        near_values = dot(hot, values[0]) + dot(hot, values[1])
        where = dot(hot, place_scratch[...], NT)
        gap = where + pltpu.roll(where, lanes - 4, 1) + pltpu.roll(where, lanes - 8, 1)
        gap = gap.reshape(chunk, atoms, lanes) - own_place[None]
        gap = jnp.where((lane < 3)[None], gap, 0.0)
        distance = jnp.sqrt(jnp.sum(gap * gap, axis=2, keepdims=True) + SOFTEN)
        scaled = (distance - centres[None]) * (1.0 / spread)
        inner = jnp.where(
            (lane < basis_count)[None],
            jnp.exp(-scaled * scaled),
            where.reshape(chunk, atoms, lanes),
        ).reshape(rows, lanes)
        before = dot3(split(inner), first).reshape(chunk, atoms, channels) + own_before[None]
        hidden = (before / (1.0 + jnp.exp(-before))).reshape(rows, channels)
        filters = dot3(split(hidden), mixing)
        total = total + jnp.sum((filters * near_values).reshape(chunk, atoms, channels), axis=0)
    out_ref[...] = total * (1.0 / math.sqrt(slots))


def call(kernel, out_shape, operands, flops, scratch=(), room=24, specs=None):
    moved = sum(x.size * 4 for x in operands)
    if specs is None:
        specs = [pl.BlockSpec(memory_space=pltpu.VMEM)] * len(operands)
    return pl.pallas_call(
        kernel,
        out_shape=out_shape,
        in_specs=specs,
        scratch_shapes=list(scratch),
        compiler_params=pltpu.CompilerParams(vmem_limit_bytes=room * 2**20),
        cost_estimate=pl.CostEstimate(flops=flops, bytes_accessed=moved, transcendentals=0),
    )(*operands)


def shift(x, axis, by):
    count = lax.axis_size(axis)
    return lax.ppermute(x, axis, [(i, (i + by) % count) for i in range(count)])


def swap(x, first=0):
    count = lax.axis_size("gx")
    one = [((i + first) % count, (i + first + 1) % count) for i in range(0, count, 2)]
    return lax.ppermute(x, "gx", one + [(b, a) for a, b in one])


def shards(
    features,
    offsets,
    species,
    neighbours,
    edge_mask,
    wavevectors,
    value_weight,
    radial_weight,
    species_embed,
    mixing_weight,
    group_filter,
):
    span0 = lax.axis_size("gx")
    span1 = lax.axis_size("gy")
    atoms, channels = features.shape[2:]
    slots = neighbours.shape[3]
    modes = wavevectors.shape[1]
    basis_count, kinds = radial_weight.shape[0], species_embed.shape[0]
    sizes = (atoms, channels, span0, span1, modes // span0)
    pairs = span0 // 2
    width = channels // span1

    distinct = distinct_triples(span0, span1)
    canonical = len(distinct) < modes
    vectors = (wavevectors,)
    rows = modes // 2
    if canonical:
        rows = -(-len(distinct) // 16) * 8
        basis = np.full((2 * rows, 8), 99.0, np.float32)
        basis[: len(distinct), :3] = distinct
        vectors = (wavevectors, jnp.asarray(basis.reshape(2, rows, 8)))

    anywhere = pl.BlockSpec(memory_space=pltpu.HBM)
    packed_shape = (atoms + EXTRA, channels)
    packed, weights = call(
        functools.partial(pack_kernel, sizes),
        [
            jax.ShapeDtypeStruct(packed_shape, F32),
            jax.ShapeDtypeStruct((width, channels), F32),
        ],
        tuple(
            pltpu.with_memory_space_constraint(x, pltpu.HBM)
            for x in (features, jnp.transpose(offsets, (0, 2, 1, 3)), species, group_filter)
        ),
        10**6,
        (
            pltpu.VMEM((3, 1, atoms), F32),
            pltpu.VMEM((1, atoms), jnp.int32),
            pltpu.SemaphoreType.DMA((4,)),
        ),
        specs=[anywhere] * 4,
    )
    column = [packed] + [shift(packed, "gy", k) for k in range(1, span1)]
    across = swap(packed, first=1)
    weights = [weights] + [shift(weights, "gx", -2 * k) for k in range(1, pairs)]

    own = call(join_kernel, jax.ShapeDtypeStruct((span1, *packed_shape), F32), column, 10**6)
    pair = swap(own)
    total = call(
        functools.partial(structure_kernel, sizes, rows, canonical),
        jax.ShapeDtypeStruct((rows, 2 * width), F32),
        (own, pair, *vectors),
        24 * rows * span1 * atoms * channels,
    )
    totals = [total] + [shift(total, "gx", 2 * k) for k in range(1, pairs)]
    weights = call(join_kernel, jax.ShapeDtypeStruct((pairs, width, channels), F32), weights, 10**6)
    pair_weights = swap(weights)
    left = shift(across, "gy", 1)
    right = shift(across, "gy", -1)

    table = jax.ShapeDtypeStruct((span1 * atoms, 4 * rows), BF16)
    high, low = call(
        functools.partial(table_kernel, sizes, rows, canonical), [table] * 2, (own, *vectors), 10**8
    )
    filtered = call(
        functools.partial(filter_kernel, sizes, rows, canonical),
        jax.ShapeDtypeStruct((2 * rows, channels), F32),
        (*totals, weights, pair_weights, *vectors),
        12 * rows * span0 * width * channels,
    )
    pair_filtered = swap(filtered)

    lanes = -(-(basis_count + kinds) // 128) * 128
    edge_sizes = (atoms, channels, span0, span1, slots, basis_count, kinds, lanes)
    nearby = call(
        functools.partial(edge_kernel, edge_sizes),
        jax.ShapeDtypeStruct((atoms, channels), F32),
        (
            own,
            pair,
            across,
            left,
            right,
            jnp.transpose(neighbours[0, 0]),
            jnp.transpose(edge_mask[0, 0]),
            value_weight,
            radial_weight,
            species_embed,
            mixing_weight,
        ),
        4 * 10**9,
        (
            pltpu.VMEM((9 * atoms, channels), F32),
            pltpu.VMEM((lanes, 9 * atoms), BF16),
            pltpu.VMEM((slots * atoms, 9 * atoms), BF16),
        ),
        24,
    )

    block = jax.ShapeDtypeStruct((atoms, channels), F32)
    scale = 1.0 / math.sqrt(atoms * span0 * span1 * modes)
    distant = call(
        functools.partial(project_kernel, sizes, scale),
        [block] * span1,
        (filtered, pair_filtered, high, low),
        24 * rows * span1 * atoms * channels,
    )
    result = nearby + distant[0]
    for k in range(1, span1):
        result = result + shift(distant[k], "gy", -k)
    return result[None, None]


def solution(mesh):
    placed = (
        P("gx", "gy", None, None),
        P("gx", "gy", None, None),
        P("gx", "gy", None),
        P("gx", "gy", None, None),
        P("gx", "gy", None, None),
        P(),
        P(),
        P(),
        P(),
        P(),
        P("gx", None, None),
    )
    return jax.shard_map(
        shards, mesh=mesh, in_specs=placed, out_specs=P("gx", "gy", None, None), check_vma=False
    )
```

```python
import functools
import math

import jax
import jax.numpy as jnp
import numpy as np
from jax import lax
from jax.experimental import pallas as pl
from jax.experimental.pallas import tpu as pltpu
from jax.sharding import PartitionSpec as P


FULL_TURN = 2.0 * math.pi
SMEARING = 0.01
RADIAL_REACH = 3.0
SOFTEN = 0.01
VERTICAL = 2
F32 = jnp.float32
BF16 = jnp.bfloat16
EXTRA = 8
NN = (((1,), (0,)), ((), ()))
NT = (((1,), (1,)), ((), ()))


def series(function):
    nodes = 0.125 + 0.125 * np.cos(np.pi * (np.arange(64) + 0.5) / 64)
    fit = np.polynomial.chebyshev.Chebyshev.fit(nodes, function(np.sqrt(nodes)), 8, domain=[0, 0.25])
    return [float(c) for c in fit.convert(kind=np.polynomial.Polynomial).coef]


COSINE = series(lambda r: np.cos(2 * np.pi * r))
SINE = series(lambda r: np.sin(2 * np.pi * r) / r)


def horner(coefficients, z):
    total = jnp.full_like(z, coefficients[-1])
    for c in coefficients[-2::-1]:
        total = total * z + c
    return total


def cos_sin(turns):
    r = turns - jnp.floor(turns + 0.5)
    z = r * r
    return horner(COSINE, z), horner(SINE, z) * r


def dot(a, b, dims=NN):
    return lax.dot_general(a, b, dims, preferred_element_type=F32)


def split(x):
    high = x.astype(BF16)
    return high, (x - high.astype(F32)).astype(BF16)


def dot3(a, b):
    a_high, a_low = a
    b_high, b_low = b
    return dot(a_high, b_high) + dot(a_low, b_high) + dot(a_high, b_low)


def quotient(x, n):
    return jnp.floor((x + 0.5) * (1.0 / n))


def iota(shape, dim):
    return lax.broadcasted_iota(jnp.int32, shape, dim)


def component(block, atoms, channels, which):
    row, lane = divmod(which * atoms, channels)
    return block[atoms + row : atoms + row + 1, lane : lane + atoms]


def mode_columns(vectors, picks):
    rows, modes = picks.shape[0], vectors.shape[1]
    chosen = (iota((rows, modes), 1).astype(F32) == picks).astype(BF16)
    padded = jnp.concatenate([vectors, jnp.zeros((5, modes), F32)], axis=0).astype(BF16)
    triples = dot(chosen, padded, NT)
    return [triples[:, n : n + 1] for n in range(3)]


def distinct_triples(span0, span1):
    kept = {}
    for n0 in range(-(span0 // 2), span0 - span0 // 2):
        for n1 in range(-(span1 // 2), span1 - span1 // 2):
            for n2 in range(-VERTICAL, VERTICAL + 1):
                if (-n0, -n1, -n2) not in kept:
                    kept[(n0, n1, n2)] = None
    return list(kept)


def key_of(n0, n1, n2):
    return jnp.abs(n0 + 128.0 * n1 + 16384.0 * n2)


def rows_of(basis_ref, vectors_ref, rows, parity):
    if basis_ref is None:
        picks = parity.astype(F32) * rows + iota((rows, 1), 0).astype(F32)
        return mode_columns(vectors_ref[...].astype(F32), picks)
    triples = basis_ref[parity]
    return [triples[:, n : n + 1] for n in range(3)]


def phases(sizes, triples, lateral, transverse, packed):
    atoms, channels, span0, span1 = sizes[:4]
    n0, n1, n2 = triples
    whole0 = n0 * lateral
    whole0 = (whole0 - span0 * quotient(whole0, span0)) * (1.0 / span0)
    whole1 = n1 * transverse
    whole1 = (whole1 - span1 * quotient(whole1, span1)) * (1.0 / span1)
    u = [component(packed, atoms, channels, n) for n in range(3)]
    turns = whole0 + whole1 + n0 * (1.0 / span0) * u[0] + n1 * (1.0 / span1) * u[1] + n2 * u[2]
    return cos_sin(turns)


def place():
    lateral, transverse = lax.axis_index("gx"), lax.axis_index("gy")
    parity = lax.rem(lateral, 2)
    return lateral.astype(F32), transverse.astype(F32), parity


def pack_kernel(sizes, features_ref, offsets_ref, species_ref, weight_ref, *refs):
    atoms, channels, _, span1 = sizes[:4]
    *refs, offsets_scratch, species_scratch, sems = refs
    tables = len(refs) // 2 - 1
    sources, out_ref, rows_ref, copies_to = refs[:tables], refs[tables], refs[tables + 1], refs[tables + 2 :]
    width = channels // span1
    start = pl.multiple_of(lax.axis_index("gy") * width, math.gcd(width, 8))
    copies = [
        pltpu.make_async_copy(offsets_ref.at[0], offsets_scratch, sems.at[0]),
        pltpu.make_async_copy(species_ref.at[0], species_scratch, sems.at[1]),
        pltpu.make_async_copy(features_ref.at[0, 0], out_ref.at[0:atoms], sems.at[2]),
        pltpu.make_async_copy(weight_ref.at[0, pl.ds(start, width)], rows_ref, sems.at[3]),
    ]
    for n, (source, target) in enumerate(zip(sources, copies_to)):
        copies.append(pltpu.make_async_copy(source, target, sems.at[4 + n]))
    for copy in copies:
        copy.start()
    out_ref[atoms:] = jnp.zeros((EXTRA, channels), F32)
    for copy in copies[:2]:
        copy.wait()
    for which in range(4):
        row, lane = divmod(which * atoms, channels)
        source = offsets_scratch[which] if which < 3 else species_scratch[...].astype(F32)
        out_ref[atoms + row : atoms + row + 1, lane : lane + atoms] = source
    for copy in copies[2:]:
        copy.wait()


def join_kernel(*refs):
    for n, ref in enumerate(refs[:-1]):
        refs[-1][n] = ref[...]


def column_kernel(*refs):
    blocks, (own_ref, sides_ref) = refs[:-2], refs[-2:]
    for n, ref in enumerate(blocks):
        own_ref[n] = ref[...]
    sides_ref[0] = blocks[1][...]
    sides_ref[1] = blocks[-1][...]


def structure_kernel(sizes, rows, canonical, paired, *refs):
    atoms, channels, _, span1 = sizes[:4]
    blocks_ref, vectors_ref = refs[:2]
    basis_ref, out_ref = refs[2] if canonical else None, refs[-1]
    lateral, transverse, parity = place()
    triples = rows_of(basis_ref, vectors_ref, rows, parity)
    row = lateral + 1.0 - 2.0 * parity.astype(F32) if paired else lateral
    cosines, sines = [], []
    for back in range(span1):
        cosine, sine = phases(sizes, triples, row, transverse - back, blocks_ref.at[back])
        cosines.append(cosine)
        sines.append(sine)
    table = jnp.concatenate(
        [jnp.concatenate(cosines, axis=1), jnp.concatenate(sines, axis=1)], axis=0
    )
    features = jnp.concatenate([blocks_ref[back, :atoms] for back in range(span1)], axis=0)
    sums = dot3(split(table), split(features))
    width = channels // span1
    for half in range(2):
        part = sums[half * rows : (half + 1) * rows]
        mine = jnp.zeros((rows, width), F32)
        for c in range(span1):
            mine = jnp.where(transverse == c, part[:, c * width : (c + 1) * width], mine)
        at = slice(half * width, (half + 1) * width)
        out_ref[:, at] = mine + refs[-2][:, at] if paired else mine


def table_kernel(sizes, rows, canonical, *refs):
    atoms, _, span0, span1, group = sizes
    own_ref, vectors_ref = refs[:2]
    basis_ref, (high_ref, low_ref, weight_ref) = refs[2] if canonical else None, refs[-3:]
    lateral, transverse, parity = place()
    sides = [rows_of(basis_ref, vectors_ref, rows, p) for p in (parity, 1 - parity)]
    for back in range(span1):
        packed = own_ref.at[back]
        parts = []
        for triples in sides:
            parts.extend(phases(sizes, triples, lateral, transverse - back, packed))
        at = slice(back * atoms, (back + 1) * atoms)
        high_ref[at], low_ref[at] = split(jnp.transpose(jnp.concatenate(parts, axis=0)))

    n0, n1, n2 = sides[0]
    waves = (FULL_TURN * n0 / span0, FULL_TURN * n1 / span1, FULL_TURN * n2)
    damp = jnp.exp(-SMEARING * sum(w * w for w in waves))
    pairs = span0 // 2
    number = iota((1, span0), 1).astype(F32)
    side = quotient(number, pairs)
    turn = number - pairs * side
    kind = parity.astype(F32)
    row = quotient(lateral, 2) + turn
    row = 2.0 * (row - pairs * quotient(row, pairs)) + jnp.where(side == 0.0, kind, 1.0 - kind)
    modes = vectors_ref.shape[1]
    if canonical:
        listed = vectors_ref[...].astype(F32)
        keys = key_of(listed[0:1], listed[1:2], listed[2:3])
        matches = (key_of(n0, n1, n2) == keys).astype(BF16)
        groups = quotient(iota((modes, span0), 0).astype(F32), group)
        counts = dot(matches, (groups == row).astype(BF16))
    else:
        picks = kind * rows + iota((rows, 1), 0).astype(F32)
        counts = (quotient(picks, group) == row).astype(F32)
    weight_ref[...] = counts * damp


def filter_kernel(sizes, *refs):
    channels, span0, span1 = sizes[1:4]
    pairs = span0 // 2
    sums, (own_ref, pair_ref, weight_ref, out_ref) = refs[:pairs], refs[pairs:]
    total = sums[0][...]
    for ref in sums[1:]:
        total = total + ref[...]
    width = channels // span1
    weights = weight_ref[...]
    mixed = None
    for side, ref in enumerate((own_ref, pair_ref)):
        at = range(side * pairs, (side + 1) * pairs)
        both = jnp.concatenate(
            [
                jnp.concatenate([total[:, :width] * weights[:, n : n + 1] for n in at], axis=1),
                jnp.concatenate([total[:, width:] * weights[:, n : n + 1] for n in at], axis=1),
            ],
            axis=0,
        )
        part = dot3(split(both), split(ref[...].reshape(pairs * width, channels)))
        mixed = part if mixed is None else mixed + part
    out_ref[...] = mixed


def project_kernel(sizes, scale, own_ref, pair_ref, high_ref, low_ref, *outs):
    atoms, span1 = sizes[0], sizes[3]
    filtered = split(jnp.concatenate([own_ref[...], pair_ref[...]], axis=0) * scale)
    everything = dot3((high_ref[...], low_ref[...]), filtered)
    for back in range(span1):
        outs[back][...] = everything[back * atoms : (back + 1) * atoms]


def hot_kernel(sizes, listed_ref, mask_ref, out_ref):
    atoms, _, span0, span1, slots = sizes[:5]
    lateral, transverse, parity = place()
    listed = listed_ref[...].astype(F32)
    source = quotient(listed, atoms)
    source0 = quotient(source, span1)
    shift0 = source0 - lateral + 1.0
    shift0 = shift0 - span0 * quotient(shift0, span0)
    shift1 = source - source0 * span1 - transverse + 1.0
    shift1 = shift1 - span1 * quotient(shift1, span1)
    line = (shift0 - 1.0) * (1.0 - 2.0 * parity.astype(F32)) + 1.0
    row = (line * 3.0 + shift1) * atoms + (listed - source * atoms)
    row = jnp.transpose(jnp.where(mask_ref[...] != 0, row, -1.0)).astype(jnp.int32)
    for slot in range(slots):
        hot = iota((atoms, 9 * atoms), 1) == row[:, slot : slot + 1]
        out_ref[slot * atoms : (slot + 1) * atoms] = jnp.where(hot, 1.0, 0.0).astype(BF16)


def edge_kernel(
    sizes,
    own_ref,
    pair_ref,
    across_ref,
    sides_ref,
    hot_ref,
    value_ref,
    radial_ref,
    embed_ref,
    mixing_ref,
    out_ref,
    feature_scratch,
    place_scratch,
):
    atoms, channels, _, span1, slots, basis_count, kinds, lanes = sizes
    parity = place()[2]
    toward = 1.0 - 2.0 * parity.astype(F32)
    last = span1 - 1
    own_rows = None
    table = (
        (sides_ref.at[0], across_ref, sides_ref.at[1]),
        (own_ref.at[1], own_ref.at[0], own_ref.at[last]),
        (pair_ref.at[1], pair_ref.at[0], pair_ref.at[last]),
    )
    low = iota((16, atoms), 0)
    kind_rows = iota((lanes - basis_count, atoms), 0)
    for r, row_refs in enumerate(table):
        for d, packed in enumerate(row_refs):
            at = (r * 3 + d) * atoms
            feature_scratch[at : at + atoms] = packed[:atoms]
            species = component(packed, atoms, channels, 3).astype(jnp.int32)
            kind_hot = jnp.where(kind_rows == species, 1.0, 0.0)
            positions = jnp.zeros((16, atoms), F32)
            exact = positions
            for n, shift in enumerate(((r - 1.0) * toward, d - 1.0, 0.0)):
                u = component(packed, atoms, channels, n)
                exact = jnp.where(low == n, u, exact)
                rest = u + shift
                for piece in range(3):
                    part = rest.astype(BF16).astype(F32)
                    positions = jnp.where(low == n + 4 * piece, part, positions)
                    rest = rest - part
            gap = jnp.zeros((basis_count - 16, atoms), F32)
            where = jnp.concatenate([positions, gap, kind_hot], axis=0)
            place_scratch[:, at : at + atoms] = where.astype(BF16)
            if r == 1 and d == 1:
                own_rows = jnp.concatenate([exact, gap, kind_hot], axis=0)

    own = jnp.transpose(own_rows)
    lane = iota((atoms, lanes), 1)
    own_place = jnp.where(lane < 3, own, 0.0)
    missing = lanes - basis_count - kinds
    first = [radial_ref[...], embed_ref[...]]
    if missing:
        first.append(jnp.zeros((missing, channels), F32))
    first = split(jnp.concatenate(first, axis=0))
    own_kind = jnp.where(lane >= basis_count, own, 0.0).astype(BF16)
    own_before = dot(own_kind, first[0]) + dot(own_kind, first[1])

    values = split(dot3(split(feature_scratch[...]), split(value_ref[...])))
    mixing = split(mixing_ref[...])
    centres = lane.astype(F32) * (RADIAL_REACH / (basis_count - 1))
    spread = 2.0 * RADIAL_REACH / (basis_count - 1)
    chunk = slots // 2
    total = jnp.zeros((atoms, channels), F32)
    for start in range(0, slots, chunk):
        rows = chunk * atoms
        hot = hot_ref[start * atoms : start * atoms + rows]
        near_values = dot(hot, values[0]) + dot(hot, values[1])
        where = dot(hot, place_scratch[...], NT)
        gap = where + pltpu.roll(where, lanes - 4, 1) + pltpu.roll(where, lanes - 8, 1)
        gap = gap.reshape(chunk, atoms, lanes) - own_place[None]
        gap = jnp.where((lane < 3)[None], gap, 0.0)
        distance = jnp.sqrt(jnp.sum(gap * gap, axis=2, keepdims=True) + SOFTEN)
        scaled = (distance - centres[None]) * (1.0 / spread)
        inner = jnp.where(
            (lane < basis_count)[None],
            jnp.exp(-scaled * scaled),
            where.reshape(chunk, atoms, lanes),
        ).reshape(rows, lanes)
        before = dot3(split(inner), first).reshape(chunk, atoms, channels) + own_before[None]
        hidden = (before / (1.0 + jnp.exp(-before))).reshape(rows, channels)
        filters = dot3(split(hidden), mixing)
        total = total + jnp.sum((filters * near_values).reshape(chunk, atoms, channels), axis=0)
    out_ref[...] = total * (1.0 / math.sqrt(slots))


def call(kernel, out_shape, operands, flops, scratch=(), room=24, specs=None):
    moved = sum(x.size * 4 for x in operands)
    if specs is None:
        specs = [pl.BlockSpec(memory_space=pltpu.VMEM)] * len(operands)
    return pl.pallas_call(
        kernel,
        out_shape=out_shape,
        in_specs=specs,
        scratch_shapes=list(scratch),
        compiler_params=pltpu.CompilerParams(vmem_limit_bytes=room * 2**20),
        cost_estimate=pl.CostEstimate(flops=flops, bytes_accessed=moved, transcendentals=0),
    )(*operands)


def shift(x, axis, by):
    count = lax.axis_size(axis)
    return lax.ppermute(x, axis, [(i, (i + by) % count) for i in range(count)])


def swap(x, first=0):
    count = lax.axis_size("gx")
    one = [((i + first) % count, (i + first + 1) % count) for i in range(0, count, 2)]
    return lax.ppermute(x, "gx", one + [(b, a) for a, b in one])


def shards(
    features,
    offsets,
    species,
    neighbours,
    edge_mask,
    wavevectors,
    value_weight,
    radial_weight,
    species_embed,
    mixing_weight,
    group_filter,
):
    span0 = lax.axis_size("gx")
    span1 = lax.axis_size("gy")
    atoms, channels = features.shape[2:]
    slots = neighbours.shape[3]
    modes = wavevectors.shape[1]
    basis_count, kinds = radial_weight.shape[0], species_embed.shape[0]
    sizes = (atoms, channels, span0, span1, modes // span0)
    pairs = span0 // 2
    width = channels // span1

    distinct = distinct_triples(span0, span1)
    canonical = len(distinct) < modes
    vectors = (wavevectors,)
    rows = modes // 2
    if canonical:
        rows = -(-len(distinct) // 16) * 8
        basis = np.full((2 * rows, 8), 99.0, np.float32)
        basis[: len(distinct), :3] = distinct
        vectors = (wavevectors, jnp.asarray(basis.reshape(2, rows, 8)))

    anywhere = pl.BlockSpec(memory_space=pltpu.HBM)
    packed_shape = (atoms + EXTRA, channels)
    packed, weights, *vectors = call(
        functools.partial(pack_kernel, sizes),
        [
            jax.ShapeDtypeStruct(packed_shape, F32),
            jax.ShapeDtypeStruct((width, channels), F32),
        ]
        + [jax.ShapeDtypeStruct(x.shape, x.dtype) for x in vectors],
        tuple(
            pltpu.with_memory_space_constraint(x, pltpu.HBM)
            for x in (features, jnp.transpose(offsets, (0, 2, 1, 3)), species, group_filter, *vectors)
        ),
        10**6,
        (
            pltpu.VMEM((3, 1, atoms), F32),
            pltpu.VMEM((1, atoms), jnp.int32),
            pltpu.SemaphoreType.DMA((6,)),
        ),
        specs=[anywhere] * (4 + len(vectors)),
    )
    column = [packed] + [shift(packed, "gy", k) for k in range(1, span1)]
    across = swap(packed, first=1)
    weights = [weights] + [shift(weights, "gx", -2 * k) for k in range(1, pairs)]

    own, sides = call(
        column_kernel,
        [
            jax.ShapeDtypeStruct((span1, *packed_shape), F32),
            jax.ShapeDtypeStruct((2, *packed_shape), F32),
        ],
        column,
        10**6,
    )
    pair = swap(own)
    partial_sum = jax.ShapeDtypeStruct((rows, 2 * width), F32)
    total = call(
        functools.partial(structure_kernel, sizes, rows, canonical, False),
        partial_sum,
        (own, *vectors),
        12 * rows * span1 * atoms * channels,
    )
    total = call(
        functools.partial(structure_kernel, sizes, rows, canonical, True),
        partial_sum,
        (pair, *vectors, total),
        12 * rows * span1 * atoms * channels,
    )
    totals = [total] + [shift(total, "gx", 2 * k) for k in range(1, pairs)]
    weights = call(join_kernel, jax.ShapeDtypeStruct((pairs, width, channels), F32), weights, 10**6)
    pair_weights = swap(weights)
    sides = swap(sides, first=1)

    table = jax.ShapeDtypeStruct((span1 * atoms, 4 * rows), BF16)
    high, low, shares = call(
        functools.partial(table_kernel, sizes, rows, canonical),
        [table, table, jax.ShapeDtypeStruct((rows, span0), F32)],
        (own, *vectors),
        10**8,
    )
    filtered = call(
        functools.partial(filter_kernel, sizes),
        jax.ShapeDtypeStruct((2 * rows, channels), F32),
        (*totals, weights, pair_weights, shares),
        12 * rows * span0 * width * channels,
    )
    pair_filtered = swap(filtered)

    lanes = -(-(basis_count + kinds) // 128) * 128
    edge_sizes = (atoms, channels, span0, span1, slots, basis_count, kinds, lanes)
    hot = call(
        functools.partial(hot_kernel, edge_sizes),
        jax.ShapeDtypeStruct((slots * atoms, 9 * atoms), BF16),
        (jnp.transpose(neighbours[0, 0]), jnp.transpose(edge_mask[0, 0])),
        10**8,
    )
    nearby = call(
        functools.partial(edge_kernel, edge_sizes),
        jax.ShapeDtypeStruct((atoms, channels), F32),
        (
            own,
            pair,
            across,
            sides,
            hot,
            value_weight,
            radial_weight,
            species_embed,
            mixing_weight,
        ),
        4 * 10**9,
        (
            pltpu.VMEM((9 * atoms, channels), F32),
            pltpu.VMEM((lanes, 9 * atoms), BF16),
        ),
    )

    block = jax.ShapeDtypeStruct((atoms, channels), F32)
    scale = 1.0 / math.sqrt(atoms * span0 * span1 * modes)
    distant = call(
        functools.partial(project_kernel, sizes, scale),
        [block] * span1,
        (filtered, pair_filtered, high, low),
        24 * rows * span1 * atoms * channels,
    )
    result = nearby + distant[0]
    for k in range(1, span1):
        result = result + shift(distant[k], "gy", -k)
    return result[None, None]


def solution(mesh):
    placed = (
        P("gx", "gy", None, None),
        P("gx", "gy", None, None),
        P("gx", "gy", None),
        P("gx", "gy", None, None),
        P("gx", "gy", None, None),
        P(),
        P(),
        P(),
        P(),
        P(),
        P("gx", None, None),
    )
    return jax.shard_map(
        shards, mesh=mesh, in_specs=placed, out_specs=P("gx", "gy", None, None), check_vma=False
    )
```

```python
import functools
import math

import jax
import jax.numpy as jnp
import numpy as np
from jax import lax
from jax.experimental import pallas as pl
from jax.experimental.pallas import tpu as pltpu
from jax.sharding import PartitionSpec as P


FULL_TURN = 2.0 * math.pi
SMEARING = 0.01
RADIAL_REACH = 3.0
SOFTEN = 0.01
VERTICAL = 2
F32 = jnp.float32
BF16 = jnp.bfloat16
KNOWN = 7
EXTRA = 8
NN = (((1,), (0,)), ((), ()))
NT = (((1,), (1,)), ((), ()))


def series(function):
    nodes = 0.125 + 0.125 * np.cos(np.pi * (np.arange(64) + 0.5) / 64)
    fit = np.polynomial.chebyshev.Chebyshev.fit(nodes, function(np.sqrt(nodes)), 8, domain=[0, 0.25])
    return [float(c) for c in fit.convert(kind=np.polynomial.Polynomial).coef]


COSINE = series(lambda r: np.cos(2 * np.pi * r))
SINE = series(lambda r: np.sin(2 * np.pi * r) / r)


def horner(coefficients, z):
    total = jnp.full_like(z, coefficients[-1])
    for c in coefficients[-2::-1]:
        total = total * z + c
    return total


def cos_sin(turns):
    r = turns - jnp.floor(turns + 0.5)
    z = r * r
    return horner(COSINE, z), horner(SINE, z) * r


def dot(a, b, dims=NN):
    return lax.dot_general(a, b, dims, preferred_element_type=F32)


def split(x):
    high = x.astype(BF16)
    return high, (x - high.astype(F32)).astype(BF16)


def dot3(a, b):
    a_high, a_low = a
    b_high, b_low = b
    return dot(a_high, b_high) + dot(a_low, b_high) + dot(a_high, b_low)


def quotient(x, n):
    return jnp.floor((x + 0.5) * (1.0 / n))


def iota(shape, dim):
    return lax.broadcasted_iota(jnp.int32, shape, dim)


def component(block, atoms, channels, which):
    row, lane = divmod(which * atoms, channels)
    return block[atoms + row : atoms + row + 1, lane : lane + atoms]


def mode_columns(vectors, picks):
    rows, modes = picks.shape[0], vectors.shape[1]
    chosen = (iota((rows, modes), 1).astype(F32) == picks).astype(BF16)
    padded = jnp.concatenate([vectors, jnp.zeros((5, modes), F32)], axis=0).astype(BF16)
    triples = dot(chosen, padded, NT)
    return [triples[:, n : n + 1] for n in range(3)]


def distinct_triples(span0, span1):
    kept = {}
    for n0 in range(-(span0 // 2), span0 - span0 // 2):
        for n1 in range(-(span1 // 2), span1 - span1 // 2):
            for n2 in range(-VERTICAL, VERTICAL + 1):
                if (-n0, -n1, -n2) not in kept:
                    kept[(n0, n1, n2)] = None
    return list(kept)


def key_of(n0, n1, n2):
    return jnp.abs(n0 + 128.0 * n1 + 16384.0 * n2)


def rows_of(basis_ref, vectors_ref, rows, parity):
    if basis_ref is None:
        picks = parity.astype(F32) * rows + iota((rows, 1), 0).astype(F32)
        return mode_columns(vectors_ref[...].astype(F32), picks)
    triples = basis_ref[parity]
    return [triples[:, n : n + 1] for n in range(3)]


def phases(sizes, triples, lateral, transverse, packed):
    atoms, channels, span0, span1 = sizes[:4]
    n0, n1, n2 = triples
    whole0 = n0 * lateral
    whole0 = (whole0 - span0 * quotient(whole0, span0)) * (1.0 / span0)
    whole1 = n1 * transverse
    whole1 = (whole1 - span1 * quotient(whole1, span1)) * (1.0 / span1)
    u = [component(packed, atoms, channels, n) for n in range(3)]
    turns = whole0 + whole1 + n0 * (1.0 / span0) * u[0] + n1 * (1.0 / span1) * u[1] + n2 * u[2]
    return cos_sin(turns)


def place():
    lateral, transverse = lax.axis_index("gx"), lax.axis_index("gy")
    parity = lax.rem(lateral, 2)
    return lateral.astype(F32), transverse.astype(F32), parity


def pack_kernel(sizes, features_ref, offsets_ref, species_ref, weight_ref, *refs):
    atoms, channels, _, span1 = sizes[:4]
    *refs, offsets_scratch, species_scratch, sems = refs
    tables = len(refs) // 2 - 1
    sources, out_ref, rows_ref, copies_to = refs[:tables], refs[tables], refs[tables + 1], refs[tables + 2 :]
    width = channels // span1
    start = pl.multiple_of(lax.axis_index("gy") * width, math.gcd(width, 8))
    copies = [
        pltpu.make_async_copy(offsets_ref.at[0], offsets_scratch, sems.at[0]),
        pltpu.make_async_copy(species_ref.at[0], species_scratch, sems.at[1]),
        pltpu.make_async_copy(features_ref.at[0, 0], out_ref.at[0:atoms], sems.at[2]),
        pltpu.make_async_copy(weight_ref.at[0, pl.ds(start, width)], rows_ref, sems.at[3]),
    ]
    for n, (source, target) in enumerate(zip(sources, copies_to)):
        copies.append(pltpu.make_async_copy(source, target, sems.at[4 + n]))
    for copy in copies:
        copy.start()
    out_ref[atoms:] = jnp.zeros((EXTRA, channels), F32)
    for copy in copies[:2]:
        copy.wait()
    for which in range(4):
        row, lane = divmod(which * atoms, channels)
        source = offsets_scratch[which] if which < 3 else species_scratch[...].astype(F32)
        out_ref[atoms + row : atoms + row + 1, lane : lane + atoms] = source
    for copy in copies[2:]:
        copy.wait()


def join_kernel(*refs):
    for n, ref in enumerate(refs[:-1]):
        refs[-1][n] = ref[...]


def column_kernel(*refs):
    blocks, (own_ref, sides_ref) = refs[:-2], refs[-2:]
    for n, ref in enumerate(blocks):
        own_ref[n] = ref[...]
    sides_ref[0] = blocks[1][...]
    sides_ref[1] = blocks[-1][...]


def structure_kernel(sizes, rows, canonical, paired, *refs):
    atoms, channels, _, span1 = sizes[:4]
    blocks_ref, vectors_ref = refs[:2]
    basis_ref, out_ref = refs[2] if canonical else None, refs[-1]
    lateral, transverse, parity = place()
    triples = rows_of(basis_ref, vectors_ref, rows, parity)
    row = lateral + 1.0 - 2.0 * parity.astype(F32) if paired else lateral
    cosines, sines = [], []
    for back in range(span1):
        cosine, sine = phases(sizes, triples, row, transverse - back, blocks_ref.at[back])
        cosines.append(cosine)
        sines.append(sine)
    table = jnp.concatenate(
        [jnp.concatenate(cosines, axis=1), jnp.concatenate(sines, axis=1)], axis=0
    )
    features = jnp.concatenate([blocks_ref[back, :atoms] for back in range(span1)], axis=0)
    sums = dot3(split(table), split(features))
    width = channels // span1
    for half in range(2):
        part = sums[half * rows : (half + 1) * rows]
        mine = jnp.zeros((rows, width), F32)
        for c in range(span1):
            mine = jnp.where(transverse == c, part[:, c * width : (c + 1) * width], mine)
        at = slice(half * width, (half + 1) * width)
        out_ref[:, at] = mine + refs[-2][:, at] if paired else mine


def table_kernel(sizes, rows, canonical, *refs):
    _, _, span0, span1, group = sizes
    own_ref, vectors_ref = refs[:2]
    basis_ref, (high_ref, low_ref, weight_ref) = refs[2] if canonical else None, refs[-3:]
    lateral, transverse, parity = place()
    sides = [rows_of(basis_ref, vectors_ref, rows, p) for p in (parity, 1 - parity)]
    parts = []
    for triples in sides:
        parts.extend(phases(sizes, triples, lateral, transverse, own_ref.at[0]))
    high_ref[...], low_ref[...] = split(jnp.transpose(jnp.concatenate(parts, axis=0)))

    n0, n1, n2 = sides[0]
    waves = (FULL_TURN * n0 / span0, FULL_TURN * n1 / span1, FULL_TURN * n2)
    damp = jnp.exp(-SMEARING * sum(w * w for w in waves))
    pairs = span0 // 2
    number = iota((1, span0), 1).astype(F32)
    side = quotient(number, pairs)
    turn = number - pairs * side
    kind = parity.astype(F32)
    row = quotient(lateral, 2) + turn
    row = 2.0 * (row - pairs * quotient(row, pairs)) + jnp.where(side == 0.0, kind, 1.0 - kind)
    modes = vectors_ref.shape[1]
    if canonical:
        listed = vectors_ref[...].astype(F32)
        keys = key_of(listed[0:1], listed[1:2], listed[2:3])
        matches = (key_of(n0, n1, n2) == keys).astype(BF16)
        groups = quotient(iota((modes, span0), 0).astype(F32), group)
        counts = dot(matches, (groups == row).astype(BF16))
    else:
        picks = kind * rows + iota((rows, 1), 0).astype(F32)
        counts = (quotient(picks, group) == row).astype(F32)
    weight_ref[...] = counts * damp


def filter_kernel(sizes, *refs):
    channels, span0, span1 = sizes[1:4]
    pairs = span0 // 2
    sums, (own_ref, pair_ref, weight_ref, out_ref) = refs[:pairs], refs[pairs:]
    total = sums[0][...]
    for ref in sums[1:]:
        total = total + ref[...]
    width = channels // span1
    weights = weight_ref[...]
    mixed = None
    for side, ref in enumerate((own_ref, pair_ref)):
        at = range(side * pairs, (side + 1) * pairs)
        both = jnp.concatenate(
            [
                jnp.concatenate([total[:, :width] * weights[:, n : n + 1] for n in at], axis=1),
                jnp.concatenate([total[:, width:] * weights[:, n : n + 1] for n in at], axis=1),
            ],
            axis=0,
        )
        part = dot3(split(both), split(ref[...].reshape(pairs * width, channels)))
        mixed = part if mixed is None else mixed + part
    out_ref[...] = mixed


def merge_kernel(*refs):
    total = refs[0][...]
    for ref in refs[1:-1]:
        total = total + ref[...]
    refs[-1][...] = total


def project_kernel(scale, own_ref, pair_ref, high_ref, low_ref, nearby_ref, out_ref):
    filtered = split(jnp.concatenate([own_ref[...], pair_ref[...]], axis=0) * scale)
    out_ref[...] = nearby_ref[...] + dot3((high_ref[...], low_ref[...]), filtered)


def hot_kernel(sizes, listed_ref, mask_ref, known_ref, far_ref):
    atoms, _, span0, span1, slots = sizes[:5]
    lateral, transverse, parity = place()
    listed = listed_ref[...].astype(F32)
    source = quotient(listed, atoms)
    source0 = quotient(source, span1)
    shift0 = source0 - lateral + 1.0
    shift0 = shift0 - span0 * quotient(shift0, span0)
    shift1 = source - source0 * span1 - transverse + 1.0
    shift1 = shift1 - span1 * quotient(shift1, span1)
    line = (shift0 - 1.0) * (1.0 - 2.0 * parity.astype(F32)) + 1.0
    far = jnp.where(shift1 == 1.0, 6.0, 7.0 + 0.5 * shift1)
    block = jnp.where(line == 0.0, far, (line - 1.0) * 3.0 + shift1)
    row = block * atoms + (listed - source * atoms)
    row = jnp.transpose(jnp.where(mask_ref[...] != 0, row, -1.0)).astype(jnp.int32)
    for slot in range(slots):
        at = slice(slot * atoms, (slot + 1) * atoms)
        for ref, first, count in ((known_ref, 0, KNOWN), (far_ref, KNOWN, 9 - KNOWN)):
            hot = iota((atoms, count * atoms), 1) + first * atoms == row[:, slot : slot + 1]
            ref[at] = jnp.where(hot, 1.0, 0.0).astype(BF16)


def block_rows(sizes, packed, shift0, shift1):
    atoms, channels, _, _, _, basis_count, _, lanes = sizes
    low = iota((16, atoms), 0)
    species = component(packed, atoms, channels, 3).astype(jnp.int32)
    kind_hot = jnp.where(iota((lanes - basis_count, atoms), 0) == species, 1.0, 0.0)
    positions = jnp.zeros((16, atoms), F32)
    for n, by in enumerate((shift0, shift1, 0.0)):
        rest = component(packed, atoms, channels, n) + by
        for piece in range(3):
            part = rest.astype(BF16).astype(F32)
            positions = jnp.where(low == n + 4 * piece, part, positions)
            rest = rest - part
    gap = jnp.zeros((basis_count - 16, atoms), F32)
    return jnp.concatenate([positions, gap, kind_hot], axis=0).astype(BF16)


def prepare_kernel(
    sizes, own_ref, pair_ref, across_ref, value_ref, high_ref, low_ref, place_ref
):
    atoms, span1 = sizes[0], sizes[3]
    toward = 1.0 - 2.0 * place()[2].astype(F32)
    order = (1, 0, span1 - 1)
    blocks = [(own_ref.at[n], 0.0, d - 1.0) for d, n in enumerate(order)]
    blocks += [(pair_ref.at[n], toward, d - 1.0) for d, n in enumerate(order)]
    blocks.append((across_ref, -toward, 0.0))
    for n, (packed, shift0, shift1) in enumerate(blocks):
        at = slice(n * atoms, (n + 1) * atoms)
        place_ref[:, at] = block_rows(sizes, packed, shift0, shift1)
    features = jnp.concatenate([packed[:atoms] for packed, _, _ in blocks], axis=0)
    high_ref[...], low_ref[...] = split(dot3(split(features), split(value_ref[...])))


def known_kernel(hot_ref, high_ref, low_ref, out_ref):
    hot = hot_ref[...]
    out_ref[...] = dot(hot, high_ref[...]) + dot(hot, low_ref[...])


def edge_kernel(
    sizes,
    own_ref,
    sides_ref,
    hot_ref,
    far_ref,
    place_ref,
    values_ref,
    value_ref,
    radial_ref,
    embed_ref,
    mixing_ref,
    out_ref,
):
    atoms, channels, _, _, slots, basis_count, kinds, lanes = sizes
    toward = 1.0 - 2.0 * place()[2].astype(F32)
    far_place = jnp.concatenate(
        [block_rows(sizes, sides_ref.at[n], -toward, 2.0 * n - 1.0) for n in range(2)], axis=1
    )
    far_features = jnp.concatenate([sides_ref[n, :atoms] for n in range(2)], axis=0)
    far_values = split(dot3(split(far_features), split(value_ref[...])))

    packed = own_ref.at[0]
    low = iota((lanes, atoms), 0)
    species = component(packed, atoms, channels, 3).astype(jnp.int32)
    own_rows = jnp.where(low - basis_count == species, 1.0, 0.0)
    for n in range(3):
        own_rows = jnp.where(low == n, component(packed, atoms, channels, n), own_rows)
    own = jnp.transpose(own_rows)
    lane = iota((atoms, lanes), 1)
    own_place = jnp.where(lane < 3, own, 0.0)
    missing = lanes - basis_count - kinds
    first = [radial_ref[...], embed_ref[...]]
    if missing:
        first.append(jnp.zeros((missing, channels), F32))
    first_high, first_low = split(jnp.concatenate(first, axis=0))
    first_twice = jnp.concatenate([first_high, first_high], axis=0)
    own_kind = jnp.where(lane >= basis_count, own, 0.0).astype(BF16)
    own_before = dot(own_kind, first_high) + dot(own_kind, first_low)

    mixing = split(mixing_ref[...])
    centres = lane.astype(F32) * (RADIAL_REACH / (basis_count - 1))
    spread = 2.0 * RADIAL_REACH / (basis_count - 1)
    chunk = slots // 2
    total = jnp.zeros((atoms, channels), F32)
    for start in range(0, slots, chunk):
        rows = chunk * atoms
        at = slice(start * atoms, start * atoms + rows)
        far = far_ref[at]
        near_values = values_ref[at] + dot(far, far_values[0]) + dot(far, far_values[1])
        where = dot(hot_ref[at], place_ref[...], NT) + dot(far, far_place, NT)
        gap = where + pltpu.roll(where, lanes - 4, 1) + pltpu.roll(where, lanes - 8, 1)
        gap = gap.reshape(chunk, atoms, lanes) - own_place[None]
        gap = jnp.where((lane < 3)[None], gap, 0.0)
        distance = jnp.sqrt(jnp.sum(gap * gap, axis=2, keepdims=True) + SOFTEN)
        scaled = (distance - centres[None]) * (1.0 / spread)
        inner = jnp.where(
            (lane < basis_count)[None],
            jnp.exp(-scaled * scaled),
            where.reshape(chunk, atoms, lanes),
        ).reshape(rows, lanes)
        inner_high, inner_low = split(inner)
        before = dot(jnp.concatenate([inner_high, inner_low], axis=1), first_twice)
        before = (before + dot(inner_high, first_low)).reshape(chunk, atoms, channels)
        before = before + own_before[None]
        hidden = (before / (1.0 + jnp.exp(-before))).reshape(rows, channels)
        filters = dot3(split(hidden), mixing)
        total = total + jnp.sum((filters * near_values).reshape(chunk, atoms, channels), axis=0)
    out_ref[...] = total * (1.0 / math.sqrt(slots))


def call(kernel, out_shape, operands, flops, scratch=(), room=24, specs=None):
    moved = sum(x.size * 4 for x in operands)
    if specs is None:
        specs = [pl.BlockSpec(memory_space=pltpu.VMEM)] * len(operands)
    return pl.pallas_call(
        kernel,
        out_shape=out_shape,
        in_specs=specs,
        scratch_shapes=list(scratch),
        compiler_params=pltpu.CompilerParams(vmem_limit_bytes=room * 2**20),
        cost_estimate=pl.CostEstimate(flops=flops, bytes_accessed=moved, transcendentals=0),
    )(*operands)


def shift(x, axis, by):
    count = lax.axis_size(axis)
    return lax.ppermute(x, axis, [(i, (i + by) % count) for i in range(count)])


def swap(x, first=0):
    count = lax.axis_size("gx")
    one = [((i + first) % count, (i + first + 1) % count) for i in range(0, count, 2)]
    return lax.ppermute(x, "gx", one + [(b, a) for a, b in one])


def shards(
    features,
    offsets,
    species,
    neighbours,
    edge_mask,
    wavevectors,
    value_weight,
    radial_weight,
    species_embed,
    mixing_weight,
    group_filter,
):
    span0 = lax.axis_size("gx")
    span1 = lax.axis_size("gy")
    atoms, channels = features.shape[2:]
    slots = neighbours.shape[3]
    modes = wavevectors.shape[1]
    basis_count, kinds = radial_weight.shape[0], species_embed.shape[0]
    sizes = (atoms, channels, span0, span1, modes // span0)
    pairs = span0 // 2
    width = channels // span1

    distinct = distinct_triples(span0, span1)
    canonical = len(distinct) < modes
    vectors = (wavevectors,)
    rows = modes // 2
    if canonical:
        rows = -(-len(distinct) // 16) * 8
        basis = np.full((2 * rows, 8), 99.0, np.float32)
        basis[: len(distinct), :3] = distinct
        vectors = (wavevectors, jnp.asarray(basis.reshape(2, rows, 8)))

    anywhere = pl.BlockSpec(memory_space=pltpu.HBM)
    packed_shape = (atoms + EXTRA, channels)
    packed, weights, *vectors = call(
        functools.partial(pack_kernel, sizes),
        [
            jax.ShapeDtypeStruct(packed_shape, F32),
            jax.ShapeDtypeStruct((width, channels), F32),
        ]
        + [jax.ShapeDtypeStruct(x.shape, x.dtype) for x in vectors],
        tuple(
            pltpu.with_memory_space_constraint(x, pltpu.HBM)
            for x in (features, jnp.transpose(offsets, (0, 2, 1, 3)), species, group_filter, *vectors)
        ),
        10**6,
        (
            pltpu.VMEM((3, 1, atoms), F32),
            pltpu.VMEM((1, atoms), jnp.int32),
            pltpu.SemaphoreType.DMA((6,)),
        ),
        specs=[anywhere] * (4 + len(vectors)),
    )
    column = [packed] + [shift(packed, "gy", k) for k in range(1, span1)]
    across = swap(packed, first=1)
    weights = [weights] + [shift(weights, "gx", -2 * k) for k in range(1, pairs)]

    own, sides = call(
        column_kernel,
        [
            jax.ShapeDtypeStruct((span1, *packed_shape), F32),
            jax.ShapeDtypeStruct((2, *packed_shape), F32),
        ],
        column,
        10**6,
    )
    pair = swap(own)
    partial_sum = jax.ShapeDtypeStruct((rows, 2 * width), F32)
    total = call(
        functools.partial(structure_kernel, sizes, rows, canonical, False),
        partial_sum,
        (own, *vectors),
        12 * rows * span1 * atoms * channels,
    )
    total = call(
        functools.partial(structure_kernel, sizes, rows, canonical, True),
        partial_sum,
        (pair, *vectors, total),
        12 * rows * span1 * atoms * channels,
    )
    totals = [total] + [shift(total, "gx", 2 * k) for k in range(1, pairs)]
    weights = call(join_kernel, jax.ShapeDtypeStruct((pairs, width, channels), F32), weights, 10**6)
    pair_weights = swap(weights)
    sides = swap(sides, first=1)

    table = jax.ShapeDtypeStruct((atoms, 4 * rows), BF16)
    high, low, shares = call(
        functools.partial(table_kernel, sizes, rows, canonical),
        [table, table, jax.ShapeDtypeStruct((rows, span0), F32)],
        (own, *vectors),
        10**8,
    )
    filtered = call(
        functools.partial(filter_kernel, sizes),
        jax.ShapeDtypeStruct((2 * rows, channels), F32),
        (*totals, weights, pair_weights, shares),
        12 * rows * span0 * width * channels,
    )
    quarters = [filtered] + [shift(filtered, "gy", k) for k in range(1, span1)]
    filtered = call(merge_kernel, jax.ShapeDtypeStruct((2 * rows, channels), F32), quarters, 10**6)
    pair_filtered = swap(filtered)

    lanes = -(-(basis_count + kinds) // 128) * 128
    edge_sizes = (atoms, channels, span0, span1, slots, basis_count, kinds, lanes)
    edges = slots * atoms
    hot, far = call(
        functools.partial(hot_kernel, edge_sizes),
        [
            jax.ShapeDtypeStruct((edges, KNOWN * atoms), BF16),
            jax.ShapeDtypeStruct((edges, (9 - KNOWN) * atoms), BF16),
        ],
        (jnp.transpose(neighbours[0, 0]), jnp.transpose(edge_mask[0, 0])),
        10**8,
    )
    half = jax.ShapeDtypeStruct((KNOWN * atoms, channels), BF16)
    value_high, value_low, places = call(
        functools.partial(prepare_kernel, edge_sizes),
        [half, half, jax.ShapeDtypeStruct((lanes, KNOWN * atoms), BF16)],
        (own, pair, across, value_weight),
        10**8,
    )
    near_values = call(
        known_kernel,
        jax.ShapeDtypeStruct((edges, channels), F32),
        (hot, value_high, value_low),
        10**8,
    )
    nearby = call(
        functools.partial(edge_kernel, edge_sizes),
        jax.ShapeDtypeStruct((atoms, channels), F32),
        (
            own,
            sides,
            hot,
            far,
            places,
            near_values,
            value_weight,
            radial_weight,
            species_embed,
            mixing_weight,
        ),
        4 * 10**9,
    )

    scale = 1.0 / math.sqrt(atoms * span0 * span1 * modes)
    result = call(
        functools.partial(project_kernel, scale),
        jax.ShapeDtypeStruct((atoms, channels), F32),
        (filtered, pair_filtered, high, low, nearby),
        24 * rows * atoms * channels,
    )
    return result[None, None]


def solution(mesh):
    placed = (
        P("gx", "gy", None, None),
        P("gx", "gy", None, None),
        P("gx", "gy", None),
        P("gx", "gy", None, None),
        P("gx", "gy", None, None),
        P(),
        P(),
        P(),
        P(),
        P(),
        P("gx", None, None),
    )
    return jax.shard_map(
        shards, mesh=mesh, in_specs=placed, out_specs=P("gx", "gy", None, None), check_vma=False
    )
```

```python
import functools
import math

import jax
import jax.numpy as jnp
import numpy as np
from jax import lax
from jax.experimental import pallas as pl
from jax.experimental.pallas import tpu as pltpu
from jax.sharding import PartitionSpec as P


FULL_TURN = 2.0 * math.pi
SMEARING = 0.01
RADIAL_REACH = 3.0
SOFTEN = 0.01
VERTICAL = 2
F32 = jnp.float32
BF16 = jnp.bfloat16
KNOWN = 7
EXTRA = 8
NN = (((1,), (0,)), ((), ()))
NT = (((1,), (1,)), ((), ()))


def series(function):
    nodes = 0.125 + 0.125 * np.cos(np.pi * (np.arange(64) + 0.5) / 64)
    fit = np.polynomial.chebyshev.Chebyshev.fit(nodes, function(np.sqrt(nodes)), 8, domain=[0, 0.25])
    return [float(c) for c in fit.convert(kind=np.polynomial.Polynomial).coef]


COSINE = series(lambda r: np.cos(2 * np.pi * r))
SINE = series(lambda r: np.sin(2 * np.pi * r) / r)


def horner(coefficients, z):
    total = jnp.full_like(z, coefficients[-1])
    for c in coefficients[-2::-1]:
        total = total * z + c
    return total


def cos_sin(turns):
    r = turns - jnp.floor(turns + 0.5)
    z = r * r
    return horner(COSINE, z), horner(SINE, z) * r


def dot(a, b, dims=NN):
    return lax.dot_general(a, b, dims, preferred_element_type=F32)


def split(x):
    high = x.astype(BF16)
    return high, (x - high.astype(F32)).astype(BF16)


def dot3(a, b):
    a_high, a_low = a
    b_high, b_low = b
    return dot(a_high, b_high) + dot(a_low, b_high) + dot(a_high, b_low)


def quotient(x, n):
    return jnp.floor((x + 0.5) * (1.0 / n))


def iota(shape, dim):
    return lax.broadcasted_iota(jnp.int32, shape, dim)


def component(block, atoms, channels, which):
    row, lane = divmod(which * atoms, channels)
    return block[atoms + row : atoms + row + 1, lane : lane + atoms]


def mode_columns(vectors, picks):
    rows, modes = picks.shape[0], vectors.shape[1]
    chosen = (iota((rows, modes), 1).astype(F32) == picks).astype(BF16)
    padded = jnp.concatenate([vectors, jnp.zeros((5, modes), F32)], axis=0).astype(BF16)
    triples = dot(chosen, padded, NT)
    return [triples[:, n : n + 1] for n in range(3)]


def distinct_triples(span0, span1):
    kept = {}
    for n0 in range(-(span0 // 2), span0 - span0 // 2):
        for n1 in range(-(span1 // 2), span1 - span1 // 2):
            for n2 in range(-VERTICAL, VERTICAL + 1):
                if (-n0, -n1, -n2) not in kept:
                    kept[(n0, n1, n2)] = None
    return list(kept)


def key_of(n0, n1, n2):
    return jnp.abs(n0 + 128.0 * n1 + 16384.0 * n2)


def rows_of(basis_ref, vectors_ref, rows, parity):
    if basis_ref is None:
        picks = parity.astype(F32) * rows + iota((rows, 1), 0).astype(F32)
        return mode_columns(vectors_ref[...].astype(F32), picks)
    triples = basis_ref[parity]
    return [triples[:, n : n + 1] for n in range(3)]


def phases(sizes, triples, lateral, transverse, packed):
    atoms, channels, span0, span1 = sizes[:4]
    n0, n1, n2 = triples
    whole0 = n0 * lateral
    whole0 = (whole0 - span0 * quotient(whole0, span0)) * (1.0 / span0)
    whole1 = n1 * transverse
    whole1 = (whole1 - span1 * quotient(whole1, span1)) * (1.0 / span1)
    u = [component(packed, atoms, channels, n) for n in range(3)]
    turns = whole0 + whole1 + n0 * (1.0 / span0) * u[0] + n1 * (1.0 / span1) * u[1] + n2 * u[2]
    return cos_sin(turns)


def place():
    lateral, transverse = lax.axis_index("gx"), lax.axis_index("gy")
    parity = lax.rem(lateral, 2)
    return lateral.astype(F32), transverse.astype(F32), parity


def pack_kernel(sizes, features_ref, offsets_ref, species_ref, weight_ref, *refs):
    atoms, channels, _, span1 = sizes[:4]
    *refs, offsets_scratch, species_scratch, sems = refs
    tables = len(refs) // 2 - 1
    sources, out_ref, rows_ref, copies_to = refs[:tables], refs[tables], refs[tables + 1], refs[tables + 2 :]
    width = channels // span1
    start = pl.multiple_of(lax.axis_index("gy") * width, math.gcd(width, 8))
    copies = [
        pltpu.make_async_copy(offsets_ref.at[0], offsets_scratch, sems.at[0]),
        pltpu.make_async_copy(species_ref.at[0], species_scratch, sems.at[1]),
        pltpu.make_async_copy(features_ref.at[0, 0], out_ref.at[0:atoms], sems.at[2]),
        pltpu.make_async_copy(weight_ref.at[0, pl.ds(start, width)], rows_ref, sems.at[3]),
    ]
    for n, (source, target) in enumerate(zip(sources, copies_to)):
        copies.append(pltpu.make_async_copy(source, target, sems.at[4 + n]))
    for copy in copies:
        copy.start()
    out_ref[atoms:] = jnp.zeros((EXTRA, channels), F32)
    for copy in copies[:2]:
        copy.wait()
    for which in range(4):
        row, lane = divmod(which * atoms, channels)
        source = offsets_scratch[which] if which < 3 else species_scratch[...].astype(F32)
        out_ref[atoms + row : atoms + row + 1, lane : lane + atoms] = source
    for copy in copies[2:]:
        copy.wait()


def join_kernel(*refs):
    for n, ref in enumerate(refs[:-1]):
        refs[-1][n] = ref[...]


def column_kernel(*refs):
    blocks, (own_ref, sides_ref) = refs[:-2], refs[-2:]
    for n, ref in enumerate(blocks):
        own_ref[n] = ref[...]
    sides_ref[0] = blocks[1][...]
    sides_ref[1] = blocks[-1][...]


def structure_kernel(sizes, rows, canonical, paired, *refs):
    atoms, channels, _, span1 = sizes[:4]
    blocks_ref, vectors_ref = refs[:2]
    basis_ref, out_ref = refs[2] if canonical else None, refs[-1]
    lateral, transverse, parity = place()
    triples = rows_of(basis_ref, vectors_ref, rows, parity)
    row = lateral + 1.0 - 2.0 * parity.astype(F32) if paired else lateral
    cosines, sines = [], []
    for back in range(span1):
        cosine, sine = phases(sizes, triples, row, transverse - back, blocks_ref.at[back])
        cosines.append(cosine)
        sines.append(sine)
    table = jnp.concatenate(
        [jnp.concatenate(cosines, axis=1), jnp.concatenate(sines, axis=1)], axis=0
    )
    features = jnp.concatenate([blocks_ref[back, :atoms] for back in range(span1)], axis=0)
    sums = dot3(split(table), split(features))
    width = channels // span1
    for half in range(2):
        part = sums[half * rows : (half + 1) * rows]
        mine = jnp.zeros((rows, width), F32)
        for c in range(span1):
            mine = jnp.where(transverse == c, part[:, c * width : (c + 1) * width], mine)
        at = slice(half * width, (half + 1) * width)
        out_ref[:, at] = mine + refs[-2][:, at] if paired else mine


def table_kernel(sizes, rows, canonical, *refs):
    _, _, span0, span1, group = sizes
    own_ref, vectors_ref = refs[:2]
    basis_ref, weight_ref = refs[2] if canonical else None, refs[-1]
    halves = (refs[-5:-3], refs[-3:-1])
    lateral, transverse, parity = place()
    sides = [rows_of(basis_ref, vectors_ref, rows, p) for p in (parity, 1 - parity)]
    for triples, half in zip(sides, halves):
        parts = phases(sizes, triples, lateral, transverse, own_ref.at[0])
        half[0][...], half[1][...] = split(jnp.transpose(jnp.concatenate(parts, axis=0)))

    n0, n1, n2 = sides[0]
    waves = (FULL_TURN * n0 / span0, FULL_TURN * n1 / span1, FULL_TURN * n2)
    damp = jnp.exp(-SMEARING * sum(w * w for w in waves))
    pairs = span0 // 2
    number = iota((1, span0), 1).astype(F32)
    side = quotient(number, pairs)
    turn = number - pairs * side
    kind = parity.astype(F32)
    row = quotient(lateral, 2) + turn
    row = 2.0 * (row - pairs * quotient(row, pairs)) + jnp.where(side == 0.0, kind, 1.0 - kind)
    modes = vectors_ref.shape[1]
    if canonical:
        listed = vectors_ref[...].astype(F32)
        keys = key_of(listed[0:1], listed[1:2], listed[2:3])
        matches = (key_of(n0, n1, n2) == keys).astype(BF16)
        groups = quotient(iota((modes, span0), 0).astype(F32), group)
        counts = dot(matches, (groups == row).astype(BF16))
    else:
        picks = kind * rows + iota((rows, 1), 0).astype(F32)
        counts = (quotient(picks, group) == row).astype(F32)
    weight_ref[...] = counts * damp


def filter_kernel(sizes, *refs):
    channels, span0, span1 = sizes[1:4]
    pairs = span0 // 2
    sums, (own_ref, pair_ref, weight_ref, out_ref) = refs[:pairs], refs[pairs:]
    total = sums[0][...]
    for ref in sums[1:]:
        total = total + ref[...]
    width = channels // span1
    weights = weight_ref[...]
    mixed = None
    for side, ref in enumerate((own_ref, pair_ref)):
        at = range(side * pairs, (side + 1) * pairs)
        both = jnp.concatenate(
            [
                jnp.concatenate([total[:, :width] * weights[:, n : n + 1] for n in at], axis=1),
                jnp.concatenate([total[:, width:] * weights[:, n : n + 1] for n in at], axis=1),
            ],
            axis=0,
        )
        part = dot3(split(both), split(ref[...].reshape(pairs * width, channels)))
        mixed = part if mixed is None else mixed + part
    out_ref[...] = mixed


def merge_kernel(*refs):
    total = refs[0][...]
    for ref in refs[1:-1]:
        total = total + ref[...]
    refs[-1][...] = total


def project_kernel(scale, filtered_ref, high_ref, low_ref, sum_ref, out_ref):
    filtered = split(filtered_ref[...] * scale)
    out_ref[...] = sum_ref[...] + dot3((high_ref[...], low_ref[...]), filtered)


def hot_kernel(sizes, listed_ref, mask_ref, known_ref, far_ref):
    atoms, _, span0, span1, slots = sizes[:5]
    lateral, transverse, parity = place()
    listed = listed_ref[...].astype(F32)
    source = quotient(listed, atoms)
    source0 = quotient(source, span1)
    shift0 = source0 - lateral + 1.0
    shift0 = shift0 - span0 * quotient(shift0, span0)
    shift1 = source - source0 * span1 - transverse + 1.0
    shift1 = shift1 - span1 * quotient(shift1, span1)
    line = (shift0 - 1.0) * (1.0 - 2.0 * parity.astype(F32)) + 1.0
    far = jnp.where(shift1 == 1.0, 6.0, 7.0 + 0.5 * shift1)
    block = jnp.where(line == 0.0, far, (line - 1.0) * 3.0 + shift1)
    row = block * atoms + (listed - source * atoms)
    row = jnp.transpose(jnp.where(mask_ref[...] != 0, row, -1.0)).astype(jnp.int32)
    for slot in range(slots):
        at = slice(slot * atoms, (slot + 1) * atoms)
        for ref, first, count in ((known_ref, 0, KNOWN), (far_ref, KNOWN, 9 - KNOWN)):
            hot = iota((atoms, count * atoms), 1) + first * atoms == row[:, slot : slot + 1]
            ref[at] = jnp.where(hot, 1.0, 0.0).astype(BF16)


def block_rows(sizes, packed, shift0, shift1):
    atoms, channels, _, _, _, basis_count, _, lanes = sizes
    low = iota((16, atoms), 0)
    species = component(packed, atoms, channels, 3).astype(jnp.int32)
    kind_hot = jnp.where(iota((lanes - basis_count, atoms), 0) == species, 1.0, 0.0)
    positions = jnp.zeros((16, atoms), F32)
    for n, by in enumerate((shift0, shift1, 0.0)):
        rest = component(packed, atoms, channels, n) + by
        for piece in range(3):
            part = rest.astype(BF16).astype(F32)
            positions = jnp.where(low == n + 4 * piece, part, positions)
            rest = rest - part
    gap = jnp.zeros((basis_count - 16, atoms), F32)
    return jnp.concatenate([positions, gap, kind_hot], axis=0).astype(BF16)


def prepare_kernel(
    sizes, own_ref, pair_ref, across_ref, value_ref, high_ref, low_ref, place_ref
):
    atoms, span1 = sizes[0], sizes[3]
    toward = 1.0 - 2.0 * place()[2].astype(F32)
    order = (1, 0, span1 - 1)
    blocks = [(own_ref.at[n], 0.0, d - 1.0) for d, n in enumerate(order)]
    blocks += [(pair_ref.at[n], toward, d - 1.0) for d, n in enumerate(order)]
    blocks.append((across_ref, -toward, 0.0))
    for n, (packed, shift0, shift1) in enumerate(blocks):
        at = slice(n * atoms, (n + 1) * atoms)
        place_ref[:, at] = block_rows(sizes, packed, shift0, shift1)
    features = jnp.concatenate([packed[:atoms] for packed, _, _ in blocks], axis=0)
    high_ref[...], low_ref[...] = split(dot3(split(features), split(value_ref[...])))


def known_kernel(hot_ref, high_ref, low_ref, out_ref):
    hot = hot_ref[...]
    out_ref[...] = dot(hot, high_ref[...]) + dot(hot, low_ref[...])


def edge_kernel(
    sizes,
    own_ref,
    sides_ref,
    hot_ref,
    far_ref,
    place_ref,
    values_ref,
    value_ref,
    radial_ref,
    embed_ref,
    mixing_ref,
    out_ref,
):
    atoms, channels, _, _, slots, basis_count, kinds, lanes = sizes
    toward = 1.0 - 2.0 * place()[2].astype(F32)
    far_place = jnp.concatenate(
        [block_rows(sizes, sides_ref.at[n], -toward, 2.0 * n - 1.0) for n in range(2)], axis=1
    )
    far_features = jnp.concatenate([sides_ref[n, :atoms] for n in range(2)], axis=0)
    far_values = split(dot3(split(far_features), split(value_ref[...])))

    packed = own_ref.at[0]
    low = iota((lanes, atoms), 0)
    species = component(packed, atoms, channels, 3).astype(jnp.int32)
    own_rows = jnp.where(low - basis_count == species, 1.0, 0.0)
    for n in range(3):
        own_rows = jnp.where(low == n, component(packed, atoms, channels, n), own_rows)
    own = jnp.transpose(own_rows)
    lane = iota((atoms, lanes), 1)
    own_place = jnp.where(lane < 3, own, 0.0)
    missing = lanes - basis_count - kinds
    first = [radial_ref[...], embed_ref[...]]
    if missing:
        first.append(jnp.zeros((missing, channels), F32))
    first_high, first_low = split(jnp.concatenate(first, axis=0))
    first_twice = jnp.concatenate([first_high, first_high], axis=0)
    own_kind = jnp.where(lane >= basis_count, own, 0.0).astype(BF16)
    own_before = dot(own_kind, first_high) + dot(own_kind, first_low)

    mixing = split(mixing_ref[...])
    centres = lane.astype(F32) * (RADIAL_REACH / (basis_count - 1))
    spread = 2.0 * RADIAL_REACH / (basis_count - 1)
    chunk = slots // 2
    total = jnp.zeros((atoms, channels), F32)
    for start in range(0, slots, chunk):
        rows = chunk * atoms
        at = slice(start * atoms, start * atoms + rows)
        far = far_ref[at]
        near_values = values_ref[at] + dot(far, far_values[0]) + dot(far, far_values[1])
        where = dot(hot_ref[at], place_ref[...], NT) + dot(far, far_place, NT)
        gap = where + pltpu.roll(where, lanes - 4, 1) + pltpu.roll(where, lanes - 8, 1)
        gap = gap.reshape(chunk, atoms, lanes) - own_place[None]
        gap = jnp.where((lane < 3)[None], gap, 0.0)
        distance = jnp.sqrt(jnp.sum(gap * gap, axis=2, keepdims=True) + SOFTEN)
        scaled = (distance - centres[None]) * (1.0 / spread)
        inner = jnp.where(
            (lane < basis_count)[None],
            jnp.exp(-scaled * scaled),
            where.reshape(chunk, atoms, lanes),
        ).reshape(rows, lanes)
        inner_high, inner_low = split(inner)
        before = dot(jnp.concatenate([inner_high, inner_low], axis=1), first_twice)
        before = (before + dot(inner_high, first_low)).reshape(chunk, atoms, channels)
        before = before + own_before[None]
        hidden = (before / (1.0 + jnp.exp(-before))).reshape(rows, channels)
        filters = dot3(split(hidden), mixing)
        total = total + jnp.sum((filters * near_values).reshape(chunk, atoms, channels), axis=0)
    out_ref[...] = total * (1.0 / math.sqrt(slots))


def call(kernel, out_shape, operands, flops, scratch=(), room=24, specs=None):
    moved = sum(x.size * 4 for x in operands)
    if specs is None:
        specs = [pl.BlockSpec(memory_space=pltpu.VMEM)] * len(operands)
    return pl.pallas_call(
        kernel,
        out_shape=out_shape,
        in_specs=specs,
        scratch_shapes=list(scratch),
        compiler_params=pltpu.CompilerParams(vmem_limit_bytes=room * 2**20),
        cost_estimate=pl.CostEstimate(flops=flops, bytes_accessed=moved, transcendentals=0),
    )(*operands)


def shift(x, axis, by):
    count = lax.axis_size(axis)
    return lax.ppermute(x, axis, [(i, (i + by) % count) for i in range(count)])


def swap(x, first=0):
    count = lax.axis_size("gx")
    one = [((i + first) % count, (i + first + 1) % count) for i in range(0, count, 2)]
    return lax.ppermute(x, "gx", one + [(b, a) for a, b in one])


def shards(
    features,
    offsets,
    species,
    neighbours,
    edge_mask,
    wavevectors,
    value_weight,
    radial_weight,
    species_embed,
    mixing_weight,
    group_filter,
):
    span0 = lax.axis_size("gx")
    span1 = lax.axis_size("gy")
    atoms, channels = features.shape[2:]
    slots = neighbours.shape[3]
    modes = wavevectors.shape[1]
    basis_count, kinds = radial_weight.shape[0], species_embed.shape[0]
    sizes = (atoms, channels, span0, span1, modes // span0)
    pairs = span0 // 2
    width = channels // span1

    distinct = distinct_triples(span0, span1)
    canonical = len(distinct) < modes
    vectors = (wavevectors,)
    rows = modes // 2
    if canonical:
        rows = -(-len(distinct) // 16) * 8
        basis = np.full((2 * rows, 8), 99.0, np.float32)
        basis[: len(distinct), :3] = distinct
        vectors = (wavevectors, jnp.asarray(basis.reshape(2, rows, 8)))

    anywhere = pl.BlockSpec(memory_space=pltpu.HBM)
    packed_shape = (atoms + EXTRA, channels)
    packed, weights, *vectors = call(
        functools.partial(pack_kernel, sizes),
        [
            jax.ShapeDtypeStruct(packed_shape, F32),
            jax.ShapeDtypeStruct((width, channels), F32),
        ]
        + [jax.ShapeDtypeStruct(x.shape, x.dtype) for x in vectors],
        tuple(
            pltpu.with_memory_space_constraint(x, pltpu.HBM)
            for x in (features, jnp.transpose(offsets, (0, 2, 1, 3)), species, group_filter, *vectors)
        ),
        10**6,
        (
            pltpu.VMEM((3, 1, atoms), F32),
            pltpu.VMEM((1, atoms), jnp.int32),
            pltpu.SemaphoreType.DMA((6,)),
        ),
        specs=[anywhere] * (4 + len(vectors)),
    )
    column = [packed] + [shift(packed, "gy", k) for k in range(1, span1)]
    across = swap(packed, first=1)
    weights = [weights] + [shift(weights, "gx", -2 * k) for k in range(1, pairs)]

    own, sides = call(
        column_kernel,
        [
            jax.ShapeDtypeStruct((span1, *packed_shape), F32),
            jax.ShapeDtypeStruct((2, *packed_shape), F32),
        ],
        column,
        10**6,
    )
    pair = swap(own)
    partial_sum = jax.ShapeDtypeStruct((rows, 2 * width), F32)
    total = call(
        functools.partial(structure_kernel, sizes, rows, canonical, False),
        partial_sum,
        (own, *vectors),
        12 * rows * span1 * atoms * channels,
    )
    total = call(
        functools.partial(structure_kernel, sizes, rows, canonical, True),
        partial_sum,
        (pair, *vectors, total),
        12 * rows * span1 * atoms * channels,
    )
    totals = [total] + [shift(total, "gx", 2 * k) for k in range(1, pairs)]
    weights = call(join_kernel, jax.ShapeDtypeStruct((pairs, width, channels), F32), weights, 10**6)
    pair_weights = swap(weights)
    sides = swap(sides, first=1)

    table = jax.ShapeDtypeStruct((atoms, 2 * rows), BF16)
    *halves, shares = call(
        functools.partial(table_kernel, sizes, rows, canonical),
        [table] * 4 + [jax.ShapeDtypeStruct((rows, span0), F32)],
        (own, *vectors),
        10**8,
    )
    filtered = call(
        functools.partial(filter_kernel, sizes),
        jax.ShapeDtypeStruct((2 * rows, channels), F32),
        (*totals, weights, pair_weights, shares),
        12 * rows * span0 * width * channels,
    )
    quarters = [filtered] + [shift(filtered, "gy", k) for k in range(1, span1)]
    filtered = call(merge_kernel, jax.ShapeDtypeStruct((2 * rows, channels), F32), quarters, 10**6)
    pair_filtered = swap(filtered)

    lanes = -(-(basis_count + kinds) // 128) * 128
    edge_sizes = (atoms, channels, span0, span1, slots, basis_count, kinds, lanes)
    edges = slots * atoms
    hot, far = call(
        functools.partial(hot_kernel, edge_sizes),
        [
            jax.ShapeDtypeStruct((edges, KNOWN * atoms), BF16),
            jax.ShapeDtypeStruct((edges, (9 - KNOWN) * atoms), BF16),
        ],
        (jnp.transpose(neighbours[0, 0]), jnp.transpose(edge_mask[0, 0])),
        10**8,
    )
    half = jax.ShapeDtypeStruct((KNOWN * atoms, channels), BF16)
    value_high, value_low, places = call(
        functools.partial(prepare_kernel, edge_sizes),
        [half, half, jax.ShapeDtypeStruct((lanes, KNOWN * atoms), BF16)],
        (own, pair, across, value_weight),
        10**8,
    )
    near_values = call(
        known_kernel,
        jax.ShapeDtypeStruct((edges, channels), F32),
        (hot, value_high, value_low),
        10**8,
    )
    nearby = call(
        functools.partial(edge_kernel, edge_sizes),
        jax.ShapeDtypeStruct((atoms, channels), F32),
        (
            own,
            sides,
            hot,
            far,
            places,
            near_values,
            value_weight,
            radial_weight,
            species_embed,
            mixing_weight,
        ),
        4 * 10**9,
    )

    scale = 1.0 / math.sqrt(atoms * span0 * span1 * modes)
    result = nearby
    for half, tables in ((filtered, halves[:2]), (pair_filtered, halves[2:])):
        result = call(
            functools.partial(project_kernel, scale),
            jax.ShapeDtypeStruct((atoms, channels), F32),
            (half, *tables, result),
            12 * rows * atoms * channels,
        )
    return result[None, None]


def solution(mesh):
    placed = (
        P("gx", "gy", None, None),
        P("gx", "gy", None, None),
        P("gx", "gy", None),
        P("gx", "gy", None, None),
        P("gx", "gy", None, None),
        P(),
        P(),
        P(),
        P(),
        P(),
        P("gx", None, None),
    )
    return jax.shard_map(
        shards, mesh=mesh, in_specs=placed, out_specs=P("gx", "gy", None, None), check_vma=False
    )
```

```python
import functools
import math

import jax
import jax.numpy as jnp
import numpy as np
from jax import lax
from jax.experimental import pallas as pl
from jax.experimental.pallas import tpu as pltpu
from jax.sharding import PartitionSpec as P


FULL_TURN = 2.0 * math.pi
SMEARING = 0.01
RADIAL_REACH = 3.0
SOFTEN = 0.01
VERTICAL = 2
F32 = jnp.float32
BF16 = jnp.bfloat16
KNOWN = 7
EXTRA = 8
NN = (((1,), (0,)), ((), ()))
NT = (((1,), (1,)), ((), ()))


def series(function):
    nodes = 0.125 + 0.125 * np.cos(np.pi * (np.arange(64) + 0.5) / 64)
    fit = np.polynomial.chebyshev.Chebyshev.fit(nodes, function(np.sqrt(nodes)), 8, domain=[0, 0.25])
    return [float(c) for c in fit.convert(kind=np.polynomial.Polynomial).coef]


COSINE = series(lambda r: np.cos(2 * np.pi * r))
SINE = series(lambda r: np.sin(2 * np.pi * r) / r)


def horner(coefficients, z):
    total = jnp.full_like(z, coefficients[-1])
    for c in coefficients[-2::-1]:
        total = total * z + c
    return total


def cos_sin(turns):
    r = turns - jnp.floor(turns + 0.5)
    z = r * r
    return horner(COSINE, z), horner(SINE, z) * r


def dot(a, b, dims=NN):
    return lax.dot_general(a, b, dims, preferred_element_type=F32)


def split(x):
    high = x.astype(BF16)
    return high, (x - high.astype(F32)).astype(BF16)


def dot3(a, b):
    a_high, a_low = a
    b_high, b_low = b
    return dot(a_high, b_high) + dot(a_low, b_high) + dot(a_high, b_low)


def quotient(x, n):
    return jnp.floor((x + 0.5) * (1.0 / n))


def iota(shape, dim):
    return lax.broadcasted_iota(jnp.int32, shape, dim)


def component(block, atoms, channels, which):
    row, lane = divmod(which * atoms, channels)
    return block[atoms + row : atoms + row + 1, lane : lane + atoms]


def mode_columns(vectors, picks):
    rows, modes = picks.shape[0], vectors.shape[1]
    chosen = (iota((rows, modes), 1).astype(F32) == picks).astype(BF16)
    padded = jnp.concatenate([vectors, jnp.zeros((5, modes), F32)], axis=0).astype(BF16)
    triples = dot(chosen, padded, NT)
    return [triples[:, n : n + 1] for n in range(3)]


def distinct_triples(span0, span1):
    kept = {}
    for n0 in range(-(span0 // 2), span0 - span0 // 2):
        for n1 in range(-(span1 // 2), span1 - span1 // 2):
            for n2 in range(-VERTICAL, VERTICAL + 1):
                if (-n0, -n1, -n2) not in kept:
                    kept[(n0, n1, n2)] = None
    return list(kept)


def key_of(n0, n1, n2):
    return jnp.abs(n0 + 128.0 * n1 + 16384.0 * n2)


def rows_of(basis_ref, vectors_ref, rows, parity):
    if basis_ref is None:
        picks = parity.astype(F32) * rows + iota((rows, 1), 0).astype(F32)
        return mode_columns(vectors_ref[...].astype(F32), picks)
    triples = basis_ref[parity]
    return [triples[:, n : n + 1] for n in range(3)]


def phases(sizes, triples, lateral, transverse, packed):
    atoms, channels, span0, span1 = sizes[:4]
    n0, n1, n2 = triples
    whole0 = n0 * lateral
    whole0 = (whole0 - span0 * quotient(whole0, span0)) * (1.0 / span0)
    whole1 = n1 * transverse
    whole1 = (whole1 - span1 * quotient(whole1, span1)) * (1.0 / span1)
    u = [component(packed, atoms, channels, n) for n in range(3)]
    turns = whole0 + whole1 + n0 * (1.0 / span0) * u[0] + n1 * (1.0 / span1) * u[1] + n2 * u[2]
    return cos_sin(turns)


def place():
    lateral, transverse = lax.axis_index("gx"), lax.axis_index("gy")
    parity = lax.rem(lateral, 2)
    return lateral.astype(F32), transverse.astype(F32), parity


def pack_kernel(sizes, features_ref, offsets_ref, species_ref, weight_ref, *refs):
    atoms, channels, _, span1 = sizes[:4]
    *refs, offsets_scratch, species_scratch, sems = refs
    tables = len(refs) // 2 - 1
    sources, out_ref, rows_ref, copies_to = refs[:tables], refs[tables], refs[tables + 1], refs[tables + 2 :]
    width = channels // span1
    start = pl.multiple_of(lax.axis_index("gy") * width, math.gcd(width, 8))
    copies = [
        pltpu.make_async_copy(offsets_ref.at[0], offsets_scratch, sems.at[0]),
        pltpu.make_async_copy(species_ref.at[0], species_scratch, sems.at[1]),
        pltpu.make_async_copy(features_ref.at[0, 0], out_ref.at[0:atoms], sems.at[2]),
        pltpu.make_async_copy(weight_ref.at[0, pl.ds(start, width)], rows_ref, sems.at[3]),
    ]
    for n, (source, target) in enumerate(zip(sources, copies_to)):
        copies.append(pltpu.make_async_copy(source, target, sems.at[4 + n]))
    for copy in copies:
        copy.start()
    out_ref[atoms:] = jnp.zeros((EXTRA, channels), F32)
    for copy in copies[:2]:
        copy.wait()
    for which in range(4):
        row, lane = divmod(which * atoms, channels)
        source = offsets_scratch[which] if which < 3 else species_scratch[...].astype(F32)
        out_ref[atoms + row : atoms + row + 1, lane : lane + atoms] = source
    for copy in copies[2:]:
        copy.wait()


def join_kernel(*refs):
    for n, ref in enumerate(refs[:-1]):
        refs[-1][n] = ref[...]


def column_kernel(*refs):
    blocks, (own_ref, sides_ref) = refs[:-2], refs[-2:]
    for n, ref in enumerate(blocks):
        own_ref[n] = ref[...]
    sides_ref[0] = blocks[1][...]
    sides_ref[1] = blocks[-1][...]


def structure_kernel(sizes, rows, canonical, paired, *refs):
    atoms, channels, _, span1 = sizes[:4]
    blocks_ref, vectors_ref = refs[:2]
    basis_ref, out_ref = refs[2] if canonical else None, refs[-1]
    lateral, transverse, parity = place()
    triples = rows_of(basis_ref, vectors_ref, rows, parity)
    row = lateral + 1.0 - 2.0 * parity.astype(F32) if paired else lateral
    cosines, sines = [], []
    for back in range(span1):
        cosine, sine = phases(sizes, triples, row, transverse - back, blocks_ref.at[back])
        cosines.append(cosine)
        sines.append(sine)
    table = jnp.concatenate(
        [jnp.concatenate(cosines, axis=1), jnp.concatenate(sines, axis=1)], axis=0
    )
    features = jnp.concatenate([blocks_ref[back, :atoms] for back in range(span1)], axis=0)
    sums = dot3(split(table), split(features))
    width = channels // span1
    for half in range(2):
        part = sums[half * rows : (half + 1) * rows]
        mine = jnp.zeros((rows, width), F32)
        for c in range(span1):
            mine = jnp.where(transverse == c, part[:, c * width : (c + 1) * width], mine)
        at = slice(half * width, (half + 1) * width)
        out_ref[:, at] = mine + refs[-2][:, at] if paired else mine


def table_kernel(sizes, rows, canonical, *refs):
    _, _, span0, span1, group = sizes
    own_ref, vectors_ref = refs[:2]
    basis_ref, weight_ref = refs[2] if canonical else None, refs[-1]
    halves = (refs[-5:-3], refs[-3:-1])
    lateral, transverse, parity = place()
    sides = [rows_of(basis_ref, vectors_ref, rows, p) for p in (parity, 1 - parity)]
    for triples, half in zip(sides, halves):
        parts = phases(sizes, triples, lateral, transverse, own_ref.at[0])
        half[0][...], half[1][...] = split(jnp.transpose(jnp.concatenate(parts, axis=0)))

    n0, n1, n2 = sides[0]
    waves = (FULL_TURN * n0 / span0, FULL_TURN * n1 / span1, FULL_TURN * n2)
    damp = jnp.exp(-SMEARING * sum(w * w for w in waves))
    pairs = span0 // 2
    number = iota((1, span0), 1).astype(F32)
    side = quotient(number, pairs)
    turn = number - pairs * side
    kind = parity.astype(F32)
    row = quotient(lateral, 2) + turn
    row = 2.0 * (row - pairs * quotient(row, pairs)) + jnp.where(side == 0.0, kind, 1.0 - kind)
    modes = vectors_ref.shape[1]
    if canonical:
        listed = vectors_ref[...].astype(F32)
        keys = key_of(listed[0:1], listed[1:2], listed[2:3])
        matches = (key_of(n0, n1, n2) == keys).astype(BF16)
        groups = quotient(iota((modes, span0), 0).astype(F32), group)
        counts = dot(matches, (groups == row).astype(BF16))
    else:
        picks = kind * rows + iota((rows, 1), 0).astype(F32)
        counts = (quotient(picks, group) == row).astype(F32)
    weight_ref[...] = counts * damp


def filter_kernel(sizes, *refs):
    channels, span0, span1 = sizes[1:4]
    pairs = span0 // 2
    sums, (own_ref, pair_ref, weight_ref, out_ref) = refs[:pairs], refs[pairs:]
    total = sums[0][...]
    for ref in sums[1:]:
        total = total + ref[...]
    width = channels // span1
    weights = weight_ref[...]
    mixed = None
    for side, ref in enumerate((own_ref, pair_ref)):
        at = range(side * pairs, (side + 1) * pairs)
        both = jnp.concatenate(
            [
                jnp.concatenate([total[:, :width] * weights[:, n : n + 1] for n in at], axis=1),
                jnp.concatenate([total[:, width:] * weights[:, n : n + 1] for n in at], axis=1),
            ],
            axis=0,
        )
        part = dot3(split(both), split(ref[...].reshape(pairs * width, channels)))
        mixed = part if mixed is None else mixed + part
    out_ref[...] = mixed


def merge_kernel(*refs):
    total = refs[0][...]
    for ref in refs[1:-1]:
        total = total + ref[...]
    refs[-1][...] = total


def project_kernel(scale, filtered_ref, high_ref, low_ref, sum_ref, out_ref):
    filtered = split(filtered_ref[...] * scale)
    out_ref[...] = sum_ref[...] + dot3((high_ref[...], low_ref[...]), filtered)


def hot_kernel(sizes, listed_ref, mask_ref, known_ref, far_ref):
    atoms, _, span0, span1, slots = sizes[:5]
    lateral, transverse, parity = place()
    listed = listed_ref[...].astype(F32)
    source = quotient(listed, atoms)
    source0 = quotient(source, span1)
    shift0 = source0 - lateral + 1.0
    shift0 = shift0 - span0 * quotient(shift0, span0)
    shift1 = source - source0 * span1 - transverse + 1.0
    shift1 = shift1 - span1 * quotient(shift1, span1)
    line = (shift0 - 1.0) * (1.0 - 2.0 * parity.astype(F32)) + 1.0
    far = jnp.where(shift1 == 1.0, 6.0, 7.0 + 0.5 * shift1)
    block = jnp.where(line == 0.0, far, (line - 1.0) * 3.0 + shift1)
    row = block * atoms + (listed - source * atoms)
    row = jnp.transpose(jnp.where(mask_ref[...] != 0, row, -1.0)).astype(jnp.int32)
    for slot in range(slots):
        at = slice(slot * atoms, (slot + 1) * atoms)
        for ref, first, count in ((known_ref, 0, KNOWN), (far_ref, KNOWN, 9 - KNOWN)):
            hot = iota((atoms, count * atoms), 1) + first * atoms == row[:, slot : slot + 1]
            ref[at] = jnp.where(hot, 1.0, 0.0).astype(BF16)


def block_rows(sizes, packed, shift0, shift1):
    atoms, channels, _, _, _, basis_count, _, lanes = sizes
    low = iota((16, atoms), 0)
    species = component(packed, atoms, channels, 3).astype(jnp.int32)
    kind_hot = jnp.where(iota((lanes - basis_count, atoms), 0) == species, 1.0, 0.0)
    positions = jnp.zeros((16, atoms), F32)
    for n, by in enumerate((shift0, shift1, 0.0)):
        rest = component(packed, atoms, channels, n) + by
        for piece in range(3):
            part = rest.astype(BF16).astype(F32)
            positions = jnp.where(low == n + 4 * piece, part, positions)
            rest = rest - part
    gap = jnp.zeros((basis_count - 16, atoms), F32)
    return jnp.concatenate([positions, gap, kind_hot], axis=0).astype(BF16)


def prepare_kernel(
    sizes, own_ref, pair_ref, across_ref, value_ref, high_ref, low_ref, place_ref
):
    atoms, span1 = sizes[0], sizes[3]
    toward = 1.0 - 2.0 * place()[2].astype(F32)
    order = (1, 0, span1 - 1)
    blocks = [(own_ref.at[n], 0.0, d - 1.0) for d, n in enumerate(order)]
    blocks += [(pair_ref.at[n], toward, d - 1.0) for d, n in enumerate(order)]
    blocks.append((across_ref, -toward, 0.0))
    for n, (packed, shift0, shift1) in enumerate(blocks):
        at = slice(n * atoms, (n + 1) * atoms)
        place_ref[:, at] = block_rows(sizes, packed, shift0, shift1)
    features = jnp.concatenate([packed[:atoms] for packed, _, _ in blocks], axis=0)
    high_ref[...], low_ref[...] = split(dot3(split(features), split(value_ref[...])))


def known_kernel(hot_ref, high_ref, low_ref, place_ref, values_ref, where_ref):
    hot = hot_ref[...]
    values_ref[...] = dot(hot, high_ref[...]) + dot(hot, low_ref[...])
    where_ref[...] = dot(hot, place_ref[...], NT)


def edge_kernel(
    sizes,
    own_ref,
    sides_ref,
    far_ref,
    where_ref,
    values_ref,
    value_ref,
    radial_ref,
    embed_ref,
    mixing_ref,
    out_ref,
):
    atoms, channels, _, _, slots, basis_count, kinds, lanes = sizes
    toward = 1.0 - 2.0 * place()[2].astype(F32)
    far_place = jnp.concatenate(
        [block_rows(sizes, sides_ref.at[n], -toward, 2.0 * n - 1.0) for n in range(2)], axis=1
    )
    far_features = jnp.concatenate([sides_ref[n, :atoms] for n in range(2)], axis=0)
    far_values = split(dot3(split(far_features), split(value_ref[...])))

    packed = own_ref.at[0]
    low = iota((lanes, atoms), 0)
    species = component(packed, atoms, channels, 3).astype(jnp.int32)
    own_rows = jnp.where(low - basis_count == species, 1.0, 0.0)
    for n in range(3):
        own_rows = jnp.where(low == n, component(packed, atoms, channels, n), own_rows)
    own = jnp.transpose(own_rows)
    lane = iota((atoms, lanes), 1)
    own_place = jnp.where(lane < 3, own, 0.0)
    missing = lanes - basis_count - kinds
    first = [radial_ref[...], embed_ref[...]]
    if missing:
        first.append(jnp.zeros((missing, channels), F32))
    first_high, first_low = split(jnp.concatenate(first, axis=0))
    first_twice = jnp.concatenate([first_high, first_high], axis=0)
    own_kind = jnp.where(lane >= basis_count, own, 0.0).astype(BF16)
    own_before = dot(own_kind, first_high) + dot(own_kind, first_low)

    mixing = split(mixing_ref[...])
    centres = lane.astype(F32) * (RADIAL_REACH / (basis_count - 1))
    spread = 2.0 * RADIAL_REACH / (basis_count - 1)
    chunk = slots // 2
    total = jnp.zeros((atoms, channels), F32)
    for start in range(0, slots, chunk):
        rows = chunk * atoms
        at = slice(start * atoms, start * atoms + rows)
        far = far_ref[at]
        near_values = values_ref[at] + dot(far, far_values[0]) + dot(far, far_values[1])
        where = where_ref[at] + dot(far, far_place, NT)
        gap = where + pltpu.roll(where, lanes - 4, 1) + pltpu.roll(where, lanes - 8, 1)
        gap = gap.reshape(chunk, atoms, lanes) - own_place[None]
        gap = jnp.where((lane < 3)[None], gap, 0.0)
        distance = jnp.sqrt(jnp.sum(gap * gap, axis=2, keepdims=True) + SOFTEN)
        scaled = (distance - centres[None]) * (1.0 / spread)
        inner = jnp.where(
            (lane < basis_count)[None],
            jnp.exp(-scaled * scaled),
            where.reshape(chunk, atoms, lanes),
        ).reshape(rows, lanes)
        inner_high, inner_low = split(inner)
        before = dot(jnp.concatenate([inner_high, inner_low], axis=1), first_twice)
        before = (before + dot(inner_high, first_low)).reshape(chunk, atoms, channels)
        before = before + own_before[None]
        hidden = (before / (1.0 + jnp.exp(-before))).reshape(rows, channels)
        filters = dot3(split(hidden), mixing)
        total = total + jnp.sum((filters * near_values).reshape(chunk, atoms, channels), axis=0)
    out_ref[...] = total * (1.0 / math.sqrt(slots))


def call(kernel, out_shape, operands, flops, scratch=(), room=24, specs=None):
    moved = sum(x.size * 4 for x in operands)
    if specs is None:
        specs = [pl.BlockSpec(memory_space=pltpu.VMEM)] * len(operands)
    return pl.pallas_call(
        kernel,
        out_shape=out_shape,
        in_specs=specs,
        scratch_shapes=list(scratch),
        compiler_params=pltpu.CompilerParams(vmem_limit_bytes=room * 2**20),
        cost_estimate=pl.CostEstimate(flops=flops, bytes_accessed=moved, transcendentals=0),
    )(*operands)


def shift(x, axis, by):
    count = lax.axis_size(axis)
    return lax.ppermute(x, axis, [(i, (i + by) % count) for i in range(count)])


def swap(x, first=0):
    count = lax.axis_size("gx")
    one = [((i + first) % count, (i + first + 1) % count) for i in range(0, count, 2)]
    return lax.ppermute(x, "gx", one + [(b, a) for a, b in one])


def shards(
    features,
    offsets,
    species,
    neighbours,
    edge_mask,
    wavevectors,
    value_weight,
    radial_weight,
    species_embed,
    mixing_weight,
    group_filter,
):
    span0 = lax.axis_size("gx")
    span1 = lax.axis_size("gy")
    atoms, channels = features.shape[2:]
    slots = neighbours.shape[3]
    modes = wavevectors.shape[1]
    basis_count, kinds = radial_weight.shape[0], species_embed.shape[0]
    sizes = (atoms, channels, span0, span1, modes // span0)
    pairs = span0 // 2
    width = channels // span1

    distinct = distinct_triples(span0, span1)
    canonical = len(distinct) < modes
    vectors = (wavevectors,)
    rows = modes // 2
    if canonical:
        rows = -(-len(distinct) // 16) * 8
        basis = np.full((2 * rows, 8), 99.0, np.float32)
        basis[: len(distinct), :3] = distinct
        vectors = (wavevectors, jnp.asarray(basis.reshape(2, rows, 8)))

    anywhere = pl.BlockSpec(memory_space=pltpu.HBM)
    packed_shape = (atoms + EXTRA, channels)
    packed, weights, *vectors = call(
        functools.partial(pack_kernel, sizes),
        [
            jax.ShapeDtypeStruct(packed_shape, F32),
            jax.ShapeDtypeStruct((width, channels), F32),
        ]
        + [jax.ShapeDtypeStruct(x.shape, x.dtype) for x in vectors],
        tuple(
            pltpu.with_memory_space_constraint(x, pltpu.HBM)
            for x in (features, jnp.transpose(offsets, (0, 2, 1, 3)), species, group_filter, *vectors)
        ),
        10**6,
        (
            pltpu.VMEM((3, 1, atoms), F32),
            pltpu.VMEM((1, atoms), jnp.int32),
            pltpu.SemaphoreType.DMA((6,)),
        ),
        specs=[anywhere] * (4 + len(vectors)),
    )
    column = [packed] + [shift(packed, "gy", k) for k in range(1, span1)]
    across = swap(packed, first=1)
    weights = [weights] + [shift(weights, "gx", -2 * k) for k in range(1, pairs)]

    own, sides = call(
        column_kernel,
        [
            jax.ShapeDtypeStruct((span1, *packed_shape), F32),
            jax.ShapeDtypeStruct((2, *packed_shape), F32),
        ],
        column,
        10**6,
    )
    pair = swap(own)
    partial_sum = jax.ShapeDtypeStruct((rows, 2 * width), F32)
    total = call(
        functools.partial(structure_kernel, sizes, rows, canonical, False),
        partial_sum,
        (own, *vectors),
        12 * rows * span1 * atoms * channels,
    )
    total = call(
        functools.partial(structure_kernel, sizes, rows, canonical, True),
        partial_sum,
        (pair, *vectors, total),
        12 * rows * span1 * atoms * channels,
    )
    totals = [total] + [shift(total, "gx", 2 * k) for k in range(1, pairs)]
    weights = call(join_kernel, jax.ShapeDtypeStruct((pairs, width, channels), F32), weights, 10**6)
    pair_weights = swap(weights)
    sides = swap(sides, first=1)

    table = jax.ShapeDtypeStruct((atoms, 2 * rows), BF16)
    *halves, shares = call(
        functools.partial(table_kernel, sizes, rows, canonical),
        [table] * 4 + [jax.ShapeDtypeStruct((rows, span0), F32)],
        (own, *vectors),
        10**8,
    )
    filtered = call(
        functools.partial(filter_kernel, sizes),
        jax.ShapeDtypeStruct((2 * rows, channels), F32),
        (*totals, weights, pair_weights, shares),
        12 * rows * span0 * width * channels,
    )
    quarters = [filtered] + [shift(filtered, "gy", k) for k in range(1, span1)]
    filtered = call(merge_kernel, jax.ShapeDtypeStruct((2 * rows, channels), F32), quarters, 10**6)
    pair_filtered = swap(filtered)

    lanes = -(-(basis_count + kinds) // 128) * 128
    edge_sizes = (atoms, channels, span0, span1, slots, basis_count, kinds, lanes)
    edges = slots * atoms
    hot, far = call(
        functools.partial(hot_kernel, edge_sizes),
        [
            jax.ShapeDtypeStruct((edges, KNOWN * atoms), BF16),
            jax.ShapeDtypeStruct((edges, (9 - KNOWN) * atoms), BF16),
        ],
        (jnp.transpose(neighbours[0, 0]), jnp.transpose(edge_mask[0, 0])),
        10**8,
    )
    half = jax.ShapeDtypeStruct((KNOWN * atoms, channels), BF16)
    value_high, value_low, places = call(
        functools.partial(prepare_kernel, edge_sizes),
        [half, half, jax.ShapeDtypeStruct((lanes, KNOWN * atoms), BF16)],
        (own, pair, across, value_weight),
        10**8,
    )
    near_values, where = call(
        known_kernel,
        [
            jax.ShapeDtypeStruct((edges, channels), F32),
            jax.ShapeDtypeStruct((edges, lanes), F32),
        ],
        (hot, value_high, value_low, places),
        10**8,
    )
    nearby = call(
        functools.partial(edge_kernel, edge_sizes),
        jax.ShapeDtypeStruct((atoms, channels), F32),
        (
            own,
            sides,
            far,
            where,
            near_values,
            value_weight,
            radial_weight,
            species_embed,
            mixing_weight,
        ),
        4 * 10**9,
    )

    scale = 1.0 / math.sqrt(atoms * span0 * span1 * modes)
    result = nearby
    for half, tables in ((filtered, halves[:2]), (pair_filtered, halves[2:])):
        result = call(
            functools.partial(project_kernel, scale),
            jax.ShapeDtypeStruct((atoms, channels), F32),
            (half, *tables, result),
            12 * rows * atoms * channels,
        )
    return result[None, None]


def solution(mesh):
    placed = (
        P("gx", "gy", None, None),
        P("gx", "gy", None, None),
        P("gx", "gy", None),
        P("gx", "gy", None, None),
        P("gx", "gy", None, None),
        P(),
        P(),
        P(),
        P(),
        P(),
        P("gx", None, None),
    )
    return jax.shard_map(
        shards, mesh=mesh, in_specs=placed, out_specs=P("gx", "gy", None, None), check_vma=False
    )
```
